128 devices in a mesh: dp: 8 (over y_lo, z), head: 16 (over x, y_hi, core).
Axes of the slice: x: 4, y: 4 (y_hi: 2, y_lo: 2; y = y_hi * 2 + y_lo), z: 4, core: 2. Of those that a mesh axis runs over, the one named last changes fastest.
Arguments:
- projected: bfloat16 [49152, 24576], P(('dp', 'head')), may hold values from -64 to 64, as said below
- weight_exp: int32 [49152], P(('dp', 'head')), may hold values from 0 to 3
- damp_exp: int32 [128], replicated, may hold values from 0 to 2
Outputs:
- whitening: float32 [128, 192, 192], P('head')
The draws below stay inside these ranges and needn't reach their ends.
Inputs may be any that keep to these rules, and one draw needn't show every extreme that they name: `projected`: real values.
All inputs are finite; a program needn't handle non-finite values.
Results may differ from the reference program's by a relative error of at most 0.0003.
Values may be sent and summed in bfloat16 or wider, within the bound.
No kernel may reach another device: no remote copies, remote signals or barrier semaphores. Data moves between devices by JAX's collectives and lax.ppermute only.
A program may use at most 192 MiB of HBM per device.

```python
import math
import jax
import jax.numpy as jnp
from jax import lax

HEADS = 64
HD = 192
TOKENS = 49152
MATS = 128


def draw_projected(key, part):
    first, second = jax.random.split(jax.random.fold_in(key, 11))
    base = jax.random.normal(first, (TOKENS, 2 * HEADS, HD), jnp.float32)
    scales = jnp.exp(jax.random.uniform(second, (2 * HEADS, HD), jnp.float32, 0.0, math.log(8.0)))
    mixed = base + 0.6 * jnp.roll(base, 1, axis=2) - 0.4 * jnp.roll(base, 5, axis=2)
    return jnp.clip((mixed * scales).reshape(TOKENS, 2 * HEADS * HD) / 4.0, -64.0, 64.0).astype(jnp.bfloat16)


def place_ends(entries, own_key, smallest, largest):
    longest = entries.shape.index(max(entries.shape))
    spots = []
    for shift in (0, 1):
        where = [jax.random.randint(jax.random.fold_in(own_key, axis), (), 0, length) for axis, length in enumerate(entries.shape)]
        where[longest] = (where[longest] + shift) % entries.shape[longest]
        spots.append(tuple(where))
    return entries.at[spots[0]].set(smallest).at[spots[1]].set(largest)


def setup_inputs(seed: int = 0) -> dict:
    seeds = jax.random.split(jax.random.key(seed), 4)
    return {
        "projected": draw_projected(jax.random.fold_in(seeds[3], 71), 0),
        "weight_exp": place_ends(jax.random.randint(seeds[1], (TOKENS,), 0, 4), jax.random.fold_in(seeds[1], 1), 0, 3).astype(jnp.int32),
        "damp_exp": place_ends(jax.random.randint(seeds[2], (MATS,), 0, 3), jax.random.fold_in(seeds[2], 1), 0, 2).astype(jnp.int32),
    }


def reference(projected, weight_exp, damp_exp):
    mats = projected.shape[1] // HD
    weights = jnp.exp2(weight_exp.astype(jnp.float32)).astype(jnp.bfloat16)
    scaled = projected * weights[:, None]
    eye = jnp.eye(HD, dtype=jnp.float32)

    def single(index):
        start = (index * HD).astype(jnp.int32)
        left = lax.dynamic_slice_in_dim(projected, start, HD, 1)
        right = lax.dynamic_slice_in_dim(scaled, start, HD, 1)
        gram = jnp.dot(left.T.astype(jnp.float32), right.astype(jnp.float32), preferred_element_type=jnp.float32) / TOKENS
        gram = 0.5 * (gram + gram.T)
        level = jnp.trace(gram) / HD + 1e-06
        damping = jnp.exp2(-damp_exp[index].astype(jnp.float32)) * level
        lower = jnp.linalg.cholesky(gram + damping * eye)
        return jax.scipy.linalg.solve_triangular(lower, eye, lower=True)
    return lax.map(single, jnp.arange(mats, dtype=jnp.int32))
```

```python
import functools

import jax
import jax.numpy as jnp
from jax import lax
from jax.experimental import pallas as pl
from jax.experimental.pallas import tpu as pltpu
from jax.sharding import PartitionSpec as P

HD = 192
HALF = 64
LANES = 128
ROWS = 152
OUT_ROWS = 192
MATS = 128
DEVICES = ("dp", "head")


def place(device):
    dp, head = divmod(device, 16)
    y_lo, z = divmod(dp, 4)
    x, y_hi, core = head // 4, head // 2 % 2, head % 2
    return x, 2 * y_hi + y_lo, z, core


def near(v):
    return v >> 1


def far(v):
    return (v >> 1) ^ (v & 1)


def cubes(stage):
    groups = {}
    for device in range(128):
        x, y, z, core = place(device)
        inner = (near(x), near(y), near(z))
        outer = (far(x), far(y), far(z))
        key, member = (inner, outer) if (core == 0) == (stage == 0) else (outer, inner)
        slot = member[0] * 4 + member[1] * 2 + member[2]
        groups.setdefault((core, key), [0] * 8)[slot] = device
    return [groups[k] for k in sorted(groups)]


def partner_pairs():
    return [(d, d ^ 1) for d in range(128)]


def owner_groups():
    return [[dp * 16 + head for dp in range(8)] for head in range(16)]


def spot(block, inner, core):
    x, y_hi = block >> 1, block & 1
    y_lo, z = inner >> 2, inner & 3
    y = 2 * y_hi + y_lo
    a = near(x) * 4 + near(y) * 2 + near(z)
    b = far(x) * 4 + far(y) * 2 + far(z)
    return jnp.where(core == 0, b * 8 + a, a * 8 + b)


def rolled(v, by):
    return pltpu.roll(v, by, 1)


def pack(full, top, diag_tile, o_ref, slot):
    pass


def gram_kernel(core_ref, x_ref, w_ref, o_ref):
    block = pl.program_id(0)
    core = core_ref[0]
    w = w_ref[...]
    w3 = jnp.concatenate([w, w, w], axis=1)
    row = lax.broadcasted_iota(jnp.int32, (HALF, LANES), 0)
    lane = lax.broadcasted_iota(jnp.int32, (HALF, LANES), 1)
    row32, lane32 = row[:32], lane[:32]
    row8 = lax.broadcasted_iota(jnp.int32, (8, LANES), 0)
    contract = (((0,), (0,)), ((), ()))

    def finish(slot, low, mid, first, last):
        o_ref[slot, 0:64] = low
        o_ref[slot, 64:128] = jnp.where(lane - HALF > row, first, mid)
        upper, lower = last[:32], last[32:]
        folded = jnp.where(lane32 - 32 > row32, rolled(upper, 32), lower)
        o_ref[slot, 128:144] = jnp.where(lane[:16] < HALF, folded[:16], rolled(folded[16:], HALF))
        diag = jnp.sum(jnp.where(lane - HALF == row, first, 0.0), axis=0, keepdims=True)
        diag += jnp.sum(jnp.where(lane32 == row32, upper, 0.0), axis=0, keepdims=True)
        o_ref[slot, 144:152] = jnp.where(row8 == 0, jnp.broadcast_to(diag, (8, LANES)), 0.0)

    for pair in range(4):
        x = x_ref[:, 384 * pair : 384 * (pair + 1)]
        xw = x * w3
        g = lax.dot_general(x[:, :256], xw[:, :256], contract, preferred_element_type=jnp.float32)
        f = lax.dot_general(x[:, 256:], xw[:, 128:], contract, preferred_element_type=jnp.float32)
        finish(
            spot(block, 2 * pair, core),
            g[128:192, :128],
            g[64:128, :128],
            rolled(g[:64, :128], HALF),
            g[128:192, 128:],
        )
        swapped = jnp.where(lane < HALF, f[64:, 128:], f[64:, :128])
        middle = jnp.where(lane < HALF, f[:64, 128:], f[:64, :128])
        finish(
            spot(block, 2 * pair + 1, core),
            rolled(swapped, HALF),
            rolled(middle, HALF),
            g[192:, 128:],
            rolled(f[64:, 128:], HALF),
        )


def grams(projected, weights, core):
    tokens = projected.shape[0]
    return pl.pallas_call(
        gram_kernel,
        grid_spec=pltpu.PrefetchScalarGridSpec(
            num_scalar_prefetch=1,
            grid=(8,),
            in_specs=[
                pl.BlockSpec((tokens, 8 * HD), lambda i, core: (0, 2 * i + core[0])),
                pl.BlockSpec((tokens, LANES), lambda i, core: (0, 0)),
            ],
            out_specs=pl.BlockSpec((64, ROWS, LANES), lambda i, core: (0, 0, 0)),
        ),
        out_shape=jax.ShapeDtypeStruct((64, ROWS, LANES), jnp.float32),
        compiler_params=pltpu.CompilerParams(dimension_semantics=("arbitrary",)),
        cost_estimate=pl.CostEstimate(flops=2 * tokens * 64 * HD * HD, bytes_accessed=15_000_000, transcendentals=0),
        name="grams",
    )(core, projected, weights)


def mm(a, b, dims=((1,), (0,))):
    return lax.dot_general(a, b, (dims, ((), ())), precision=lax.Precision.HIGHEST, preferred_element_type=jnp.float32)


def factor(block, row, lane):
    m = jnp.where(lane - HALF == row, 1.0, block)
    out = []
    for k in range(HALF):
        t = k // 8
        j = k % 8
        sub = m[0:8]
        pivot_row = sub[j : j + 1, :]
        column = jnp.broadcast_to(m[:, k : k + 1], m.shape)
        p = column[j : j + 1, :]
        out.append(pivot_row * lax.rsqrt(p))
        if k == HALF - 1:
            break
        q = pivot_row / p
        if j == 7:
            m = m[8:] - column[8:] * q
        else:
            keep = lax.broadcasted_iota(jnp.int32, (8, LANES), 0) > j
            first = m[:8] - jnp.where(keep, column[:8] * q, 0.0)
            m = jnp.concatenate([first, m[8:] - column[8:] * q], axis=0) if m.shape[0] > 8 else first
    return jnp.concatenate(out, axis=0)


def whiten_kernel(info_ref, damp_ref, g_ref, o_ref):
    tokens_total = info_ref[1]
    packed = g_ref[0]
    for i in range(1, 8):
        packed = packed + g_ref[i]
    packed = packed / tokens_total.astype(jnp.float32)
    row = lax.broadcasted_iota(jnp.int32, (HALF, LANES), 0)
    lane = lax.broadcasted_iota(jnp.int32, (HALF, LANES), 1)
    row32, lane32 = row[:32], lane[:32]
    low = packed[0:64]
    mid = packed[64:128]
    tail = packed[128:144]
    extra = jnp.broadcast_to(packed[144:145], (HALF, LANES))
    turned = rolled(mid, HALF)
    inside = lane < HALF
    upper00 = jnp.where((lane > row) & inside, turned, 0.0)
    lower11 = jnp.where((lane < row), turned, 0.0)
    diag11 = jnp.where(lane == row, turned, 0.0)
    folded = jnp.concatenate([tail, rolled(tail, HALF)], axis=0)
    h10 = jnp.where(lane32 < 32, folded, 0.0)
    fturn = rolled(folded, LANES - 32)
    hup = jnp.where((lane32 > row32) & (lane32 < 32), fturn, 0.0)
    hlow = jnp.where(lane32 < row32, fturn, 0.0)
    hdiag = jnp.where(lane32 == row32, fturn, 0.0)
    extra_turned = rolled(extra, HALF)
    diag00 = jnp.where(lane == row, extra_turned, 0.0)
    hdiag0 = jnp.where(lane32 == row32, extra[:32], 0.0)
    lower22 = jnp.concatenate([jnp.zeros((32, LANES), jnp.float32), h10 + jnp.where(lane32 >= 32, rolled(hlow, 32), 0.0)], axis=0)
    upper22 = jnp.concatenate([hup, jnp.zeros((32, LANES), jnp.float32)], axis=0)
    diag22 = jnp.concatenate([hdiag0, rolled(hdiag, 32)], axis=0)

    def flip(v):
        return jnp.concatenate([v.T[:HALF], jnp.zeros((HALF, HALF), jnp.float32)], axis=1)

    s00 = upper00 + flip(upper00) + diag00
    s11 = lower11 + flip(lower11) + diag11
    off22 = lower22 + upper22
    s22 = off22 + flip(off22) + diag22
    trace = jnp.sum(jnp.sum(diag00 + diag11 + diag22, axis=0, keepdims=True), axis=1, keepdims=True)
    scale = (1 << damp_ref[info_ref[0]]).astype(jnp.float32)
    damping = (trace / HD + 1e-6) / scale
    eye = jnp.where(lane == row, jnp.broadcast_to(damping, (HALF, LANES)), 0.0)
    s10 = mid[:, :HALF]
    s20, s21 = low[:, :HALF], low[:, HALF:]

    w0 = factor(s00 + eye, row, lane)[:, HALF:]
    u10 = mm(w0, s10, ((1,), (1,)))
    u20 = mm(w0, s20, ((1,), (1,)))
    pad = jnp.zeros((HALF, HALF), jnp.float32)
    r11 = s11 + eye - jnp.concatenate([mm(u10, u10, ((0,), (0,))), pad], axis=1)
    r21 = s21 - mm(u20, u10, ((0,), (0,)))
    w1 = factor(r11, row, lane)[:, HALF:]
    u21 = mm(w1, r21, ((1,), (1,)))
    gap = mm(u20, u20, ((0,), (0,))) + mm(u21, u21, ((0,), (0,)))
    r22 = s22 + eye - jnp.concatenate([gap, pad], axis=1)
    x10 = mm(u10, w0, ((0,), (0,)))
    w10 = -mm(w1, x10)
    x20 = mm(u20, w0, ((0,), (0,))) + mm(u21, w10, ((0,), (0,)))
    x21 = mm(u21, w1, ((0,), (0,)))
    w2 = factor(r22, row, lane)[:, HALF:]
    low_out = -mm(w2, jnp.concatenate([x20, x21], axis=1))
    o_ref[0:64] = jnp.concatenate([w0, w2], axis=1)
    o_ref[64:128] = jnp.concatenate([w10, w1], axis=1)
    o_ref[128:192] = low_out


def whiten(info, damp_exp, parts):
    return pl.pallas_call(
        whiten_kernel,
        grid_spec=pltpu.PrefetchScalarGridSpec(
            num_scalar_prefetch=2,
            grid=(1,),
            in_specs=[pl.BlockSpec((8, ROWS, LANES), lambda i, *_: (0, 0, 0))],
            out_specs=pl.BlockSpec((OUT_ROWS, LANES), lambda i, *_: (0, 0)),
        ),
        out_shape=jax.ShapeDtypeStruct((OUT_ROWS, LANES), jnp.float32),
        name="whiten",
    )(info, damp_exp, parts)


def spread_kernel(p_ref, o_ref):
    lane = lax.broadcasted_iota(jnp.int32, (HALF, LANES), 1)
    inside = lane < HALF
    for i in range(8):
        ends = p_ref[i, 0:64]
        o_ref[i, 0:64, 0:128] = jnp.where(inside, ends, 0.0)
        o_ref[i, 64:128, 0:128] = p_ref[i, 64:128]
        o_ref[i, 128:192, 0:128] = p_ref[i, 128:192]
        o_ref[i, 0:128, 128:192] = jnp.zeros((128, HALF), jnp.float32)
        o_ref[i, 128:192, 128:192] = rolled(ends, HALF)[:, :HALF]


def spread(packed):
    return pl.pallas_call(
        spread_kernel,
        grid=(1,),
        in_specs=[pl.BlockSpec((8, OUT_ROWS, LANES), lambda i: (0, 0, 0))],
        out_specs=pl.BlockSpec((8, HD, HD), lambda i: (0, 0, 0)),
        out_shape=jax.ShapeDtypeStruct((8, HD, HD), jnp.float32),
        name="spread",
    )(packed)


def on_device(projected, weight_exp, damp_exp):
    dp, head = lax.axis_index("dp"), lax.axis_index("head")
    core = head % 2
    weights = jnp.exp2(weight_exp.astype(jnp.float32)).astype(jnp.bfloat16)
    weights = jnp.broadcast_to(weights[:, None], (weights.shape[0], LANES))
    theirs = grams(projected, weights, (1 - core)[None])
    received = lax.ppermute(theirs, DEVICES, partner_pairs())
    mine = grams(projected, weights, core[None])
    chip = SEND(mine + received).reshape(8, 8, ROWS, LANES)
    parts = lax.all_to_all(chip, DEVICES, 0, 0, tiled=True, axis_index_groups=cubes(0))
    cube = jnp.sum(parts.astype(jnp.float32), axis=0)
    parts = lax.all_to_all(cube, DEVICES, 0, 0, tiled=True, axis_index_groups=cubes(1))
    total = projected.shape[0] * lax.axis_size("dp") * lax.axis_size("head")
    info = jnp.stack([head * 8 + dp, jnp.int32(total)])
    factors = whiten(info, damp_exp, parts)
    gathered = lax.all_to_all(
        jnp.broadcast_to(factors[None], (8, OUT_ROWS, LANES)), DEVICES, 0, 0, tiled=True, axis_index_groups=owner_groups()
    )
    return spread(gathered)


def SEND(v):
    return v


def solution(mesh):
    return jax.shard_map(
        on_device,
        mesh=mesh,
        in_specs=(P(("dp", "head"), None), P(("dp", "head")), P()),
        out_specs=P("head", None, None),
        check_vma=False,
    )
```

```python
import jax
import jax.numpy as jnp
from jax import lax
from jax.experimental import pallas as pl
from jax.experimental.pallas import tpu as pltpu
from jax.sharding import PartitionSpec as P

HD = 192
HALF = 64
LANES = 128
ROWS = 152
OUT_ROWS = 192
TOKENS = 49152
DEVICES = ("dp", "head")


def place(device):
    dp, head = divmod(device, 16)
    y_lo, z = divmod(dp, 4)
    x, y_hi, core = head // 4, head // 2 % 2, head % 2
    return x, 2 * y_hi + y_lo, z, core


def near(v):
    return v >> 1


def far(v):
    return (v >> 1) ^ (v & 1)


def cubes(stage):
    groups = {}
    for device in range(128):
        x, y, z, core = place(device)
        inner = (near(x), near(y), near(z))
        outer = (far(x), far(y), far(z))
        key, member = (inner, outer) if (core == 0) == (stage == 0) else (outer, inner)
        first = member[0] if stage == 0 else member[0] ^ key[0]
        groups.setdefault((core, key), [0] * 8)[first * 4 + member[1] * 2 + member[2]] = device
    return [groups[k] for k in sorted(groups)]


def partner_pairs():
    return [(d, d ^ 1) for d in range(128)]


def peers(flip):
    pairs = []
    for group in cubes(0):
        pairs += [(group[i], group[i ^ flip]) for i in range(8)]
    return sorted(pairs)


def owner_groups():
    return [[dp * 16 + head for dp in range(8)] for head in range(16)]


def chunk_block(half, i):
    return (i >> 1) * 4 + half * 2 + (i & 1)


def spot(block, inner, core):
    x, y_hi = block >> 1, block & 1
    y_lo, z = inner >> 2, inner & 3
    y = 2 * y_hi + y_lo
    a, a_rest = near(x) * 4 + near(y) * 2 + near(z), near(y) * 2 + near(z)
    b, b_rest = far(x) * 4 + far(y) * 2 + far(z), far(y) * 2 + far(z)
    return jnp.where(core == 0, b * 4 + a_rest, a * 4 + b_rest)


def on_chip(v):
    return pltpu.with_memory_space_constraint(v, pltpu.VMEM)


def off_chip(v):
    return pltpu.with_memory_space_constraint(v, pltpu.HBM)


WHOLE = pl.BlockSpec(memory_space=pltpu.VMEM)


def params(mebibytes, **kwargs):
    return pltpu.CompilerParams(vmem_limit_bytes=mebibytes << 20, **kwargs)


def rolled(v, by):
    return pltpu.roll(v, by, 1)


def block_grams(x_ref, w_ref, put):
    w = w_ref[...]
    w3 = jnp.concatenate([w, w, w], axis=1)
    row = lax.broadcasted_iota(jnp.int32, (HALF, LANES), 0)
    lane = lax.broadcasted_iota(jnp.int32, (HALF, LANES), 1)
    row32, lane32 = row[:32], lane[:32]
    row16, lane16 = row[:16], lane[:16]
    row8 = row[:8]
    contract = (((0,), (0,)), ((), ()))

    def finish(index, low, mid, first, last, at):
        put(index, 0, low)
        put(index, 64, jnp.where(lane - HALF > row, first, mid))

        def moved(v, to):
            return v if to == at else rolled(v, (to - at) % LANES)

        near_half = jnp.where(lane16 - 32 > row16, moved(last[:16], 32), moved(last[32:48], 0))
        far_half = jnp.where(lane16 - 96 > row16 + 16, moved(last[16:32], 96), moved(last[48:64], HALF))
        put(index, 128, jnp.where(lane16 < HALF, near_half, far_half))
        diag = jnp.sum(jnp.where(lane - HALF == row, first, 0.0), axis=0, keepdims=True)
        small = jnp.sum(jnp.where(lane32 - at == row32, last[:32], 0.0), axis=0, keepdims=True)
        diag = jnp.broadcast_to(diag, (8, LANES)) + moved(jnp.broadcast_to(small, (8, LANES)), 0)
        put(index, 144, jnp.where(row8 == 0, diag, 0.0))

    for pair in range(4):
        x = x_ref[:, 384 * pair : 384 * (pair + 1)]
        xw = x * w3
        g = lax.dot_general(x[:, :256], xw[:, :256], contract, preferred_element_type=jnp.float32)
        f = lax.dot_general(x[:, 256:], xw[:, 128:], contract, preferred_element_type=jnp.float32)
        finish(2 * pair, g[128:192, :128], g[64:128, :128], rolled(g[:64, :128], HALF), g[128:192, 128:], 0)
        swapped = jnp.where(lane < HALF, f[64:, 128:], f[64:, :128])
        middle = jnp.where(lane < HALF, f[:64, 128:], f[:64, :128])
        finish(2 * pair + 1, rolled(swapped, HALF), rolled(middle, HALF), g[192:, 128:], f[64:, 128:], HALF)


def spread_weights(exp_ref, w_ref):
    for i in range(exp_ref.shape[0] // LANES):
        power = (1 << exp_ref[LANES * i : LANES * (i + 1)].reshape(1, LANES)).astype(jnp.float32)
        w_ref[LANES * i : LANES * (i + 1)] = jnp.broadcast_to(power, (LANES, LANES)).T.astype(jnp.bfloat16)


def their_grams_kernel(core_ref, x_ref, exp_ref, o_ref, w_ref):
    @pl.when(pl.program_id(0) == 0)
    def _():
        spread_weights(exp_ref, w_ref)

    i = pl.program_id(0)

    def put(index, start, rows):
        o_ref[8 * i + index, start : start + rows.shape[0]] = rows

    block_grams(x_ref, w_ref, put)


def their_grams(projected, weight_exp, core, half):
    tokens = projected.shape[0]
    return pl.pallas_call(
        their_grams_kernel,
        grid_spec=pltpu.PrefetchScalarGridSpec(
            num_scalar_prefetch=1,
            grid=(4,),
            in_specs=[
                pl.BlockSpec((tokens, 8 * HD), lambda i, core: (0, 2 * chunk_block(half, i) + 1 - core[0])),
                pl.BlockSpec((tokens,), lambda i, core: (0,)),
            ],
            out_specs=WHOLE,
            scratch_shapes=[pltpu.VMEM((tokens, LANES), jnp.bfloat16)],
        ),
        out_shape=pltpu.VMEM((32, ROWS, LANES), jnp.float32),
        compiler_params=params(12, dimension_semantics=("arbitrary",)),
        cost_estimate=pl.CostEstimate(flops=tokens * 64 * HD * HD, bytes_accessed=7_500_000, transcendentals=0),
        name="their_grams",
    )(core, off_chip(projected), off_chip(weight_exp))


def my_even_kernel(core_ref, spot_ref, x_ref, exp_ref, received_ref, o_ref, w_ref):
    fill_slots(0, core_ref, x_ref, exp_ref, received_ref, o_ref, w_ref)


def fill_slots(half, core_ref, x_ref, exp_ref, received_ref, o_ref, w_ref):
    i = pl.program_id(0)

    @pl.when(i == 0)
    def _():
        spread_weights(exp_ref, w_ref)

    block = chunk_block(half, i)
    slots = [spot(block, inner, core_ref[0]) for inner in range(8)]

    def put(index, start, rows):
        size = rows.shape[0]
        o_ref[slots[index], start : start + size] = rows + received_ref[8 * i + index, start : start + size]

    block_grams(x_ref, w_ref, put)


def my_odd_kernel(core_ref, spot_ref, x_ref, exp_ref, received_ref, *refs):
    outs, (w_ref, all_ref) = refs[:8], refs[8:]
    fill_slots(1, core_ref, x_ref, exp_ref, received_ref, all_ref, w_ref)

    @pl.when(pl.program_id(0) == pl.num_programs(0) - 1)
    def _():
        for flip in range(8):
            slot = spot_ref[0] ^ flip
            for i in range(4):
                outs[flip][i] = all_ref[slot * 4 + i]


def my_grams(projected, weight_exp, received, core, own_spot, half):
    tokens = projected.shape[0]

    scratch = [pltpu.VMEM((tokens, LANES), jnp.bfloat16)]
    if half:
        kernel, outs = my_odd_kernel, [WHOLE] * 8
        shapes = [pltpu.VMEM((4, ROWS, LANES), jnp.float32)] * 8
        scratch.append(pltpu.VMEM((32, ROWS, LANES), jnp.float32))
    else:
        kernel, outs = my_even_kernel, WHOLE
        shapes = pltpu.HBM((32, ROWS, LANES), jnp.float32)
    return pl.pallas_call(
        kernel,
        grid_spec=pltpu.PrefetchScalarGridSpec(
            num_scalar_prefetch=2,
            grid=(4,),
            in_specs=[
                pl.BlockSpec((tokens, 8 * HD), lambda i, core, spot: (0, 2 * chunk_block(half, i) + core[0])),
                pl.BlockSpec((tokens,), lambda i, core, spot: (0,)),
                WHOLE,
            ],
            out_specs=outs,
            scratch_shapes=scratch,
        ),
        out_shape=shapes,
        compiler_params=params(16, dimension_semantics=("arbitrary",)),
        cost_estimate=pl.CostEstimate(flops=tokens * 64 * HD * HD, bytes_accessed=10_000_000, transcendentals=0),
        name="my_grams",
    )(core, own_spot, off_chip(projected), off_chip(weight_exp), on_chip(received))


def even_kernel(even_ref, o_ref):
    total = even_ref[0, 0]
    for k in range(1, 8):
        total = total + even_ref[k, 0]
    o_ref[pl.program_id(0)] = total


def add_even(even):
    return pl.pallas_call(
        even_kernel,
        grid=(4,),
        in_specs=[pl.BlockSpec((8, 1, ROWS, LANES), lambda i: (0, i, 0, 0))],
        out_specs=WHOLE,
        out_shape=pltpu.VMEM((4, ROWS, LANES), jnp.float32),
        compiler_params=params(8, dimension_semantics=("arbitrary",)),
        cost_estimate=pl.CostEstimate(flops=6_000_000, bytes_accessed=3_000_000, transcendentals=0),
        name="add_even",
    )(off_chip(even))


def odd_kernel(even_ref, *refs):
    odd_refs, o_ref = refs[:8], refs[8]

    def one(i, carry):
        o_ref[i] = even_ref[i]
        total = odd_refs[0][i]
        for k in range(1, 8):
            total = total + odd_refs[k][i]
        o_ref[4 + i] = total
        return carry

    lax.fori_loop(0, 4, one, 0)


def add_odd(even_sum, odd):
    return pl.pallas_call(
        odd_kernel,
        in_specs=[WHOLE] * 9,
        out_specs=WHOLE,
        out_shape=pltpu.VMEM((8, ROWS, LANES), jnp.float32),
        compiler_params=params(8),
        name="add_odd",
    )(on_chip(even_sum), *[on_chip(v) for v in odd])


def mm(a, b, dims=((1,), (0,))):
    return lax.dot_general(a, b, (dims, ((), ())), precision=lax.Precision.HIGHEST, preferred_element_type=jnp.float32)


def factor(block, row, lane):
    m = jnp.where(lane - HALF == row, 1.0, block)
    tiles = [m[8 * t : 8 * t + 8] for t in range(8)]
    sub = lax.broadcasted_iota(jnp.int32, (8, LANES), 0)
    wide = lambda v: jnp.broadcast_to(v, (8, LANES))
    out = []
    for t in range(8):
        cols = {v: [wide(tiles[v][:, 8 * t + j : 8 * t + j + 1]) for j in range(8)] for v in range(t, 8)}
        c, d, q = cols[t], tiles[t], []
        for j in range(8):
            r = 1.0 / c[j][j : j + 1]
            out.append(d[j : j + 1] * lax.rsqrt(c[j][j : j + 1]))
            q.append(wide(d[j : j + 1] * r))
            below = jnp.where(sub > j, c[j], 0.0)
            d = d - below * q[j]
            for l in range(j + 1, 8):
                u = wide(c[l][j : j + 1] * r)
                c[l] = c[l] - below * u
                for v in range(t + 1, 8):
                    cols[v][l] = cols[v][l] - cols[v][j] * u
        for v in range(t + 1, 8):
            for j in range(8):
                tiles[v] = tiles[v] - cols[v][j] * q[j]
    return jnp.concatenate(out, axis=0)


def whiten_kernel(index_ref, damp_ref, g_ref, o_ref):
    packed = g_ref[0]
    for i in range(1, 8):
        packed = packed + g_ref[i]
    packed = packed / TOKENS
    row = lax.broadcasted_iota(jnp.int32, (HALF, LANES), 0)
    lane = lax.broadcasted_iota(jnp.int32, (HALF, LANES), 1)
    row32, lane32 = row[:32], lane[:32]
    low = packed[0:64]
    mid = packed[64:128]
    tail = packed[128:144]
    extra = jnp.broadcast_to(packed[144:145], (HALF, LANES))
    turned = rolled(mid, HALF)
    inside = lane < HALF
    upper00 = jnp.where((lane > row) & inside, turned, 0.0)
    lower11 = jnp.where((lane < row), turned, 0.0)
    diag11 = jnp.where(lane == row, turned, 0.0)
    folded = jnp.concatenate([tail, rolled(tail, HALF)], axis=0)
    h10 = jnp.where(lane32 < 32, folded, 0.0)
    fturn = rolled(folded, LANES - 32)
    hup = jnp.where((lane32 > row32) & (lane32 < 32), fturn, 0.0)
    hlow = jnp.where(lane32 < row32, fturn, 0.0)
    hdiag = jnp.where(lane32 == row32, fturn, 0.0)
    extra_turned = rolled(extra, HALF)
    diag00 = jnp.where(lane == row, extra_turned, 0.0)
    hdiag0 = jnp.where(lane32 == row32, extra[:32], 0.0)
    lower22 = jnp.concatenate([jnp.zeros((32, LANES), jnp.float32), h10 + jnp.where(lane32 >= 32, rolled(hlow, 32), 0.0)], axis=0)
    upper22 = jnp.concatenate([hup, jnp.zeros((32, LANES), jnp.float32)], axis=0)
    diag22 = jnp.concatenate([hdiag0, rolled(hdiag, 32)], axis=0)

    def flip(v):
        return jnp.concatenate([v.T[:HALF], jnp.zeros((HALF, HALF), jnp.float32)], axis=1)

    s00 = upper00 + flip(upper00) + diag00
    s11 = lower11 + flip(lower11) + diag11
    off22 = lower22 + upper22
    s22 = off22 + flip(off22) + diag22
    trace = jnp.sum(jnp.sum(diag00 + diag11 + diag22, axis=0, keepdims=True), axis=1, keepdims=True)
    scale = (1 << damp_ref[index_ref[0]]).astype(jnp.float32)
    damping = (trace / HD + 1e-6) / scale
    eye = jnp.where(lane == row, jnp.broadcast_to(damping, (HALF, LANES)), 0.0)
    s10 = mid[:, :HALF]
    s20, s21 = low[:, :HALF], low[:, HALF:]

    w0 = factor(s00 + eye, row, lane)[:, HALF:]
    u10 = mm(w0, s10, ((1,), (1,)))
    u20 = mm(w0, s20, ((1,), (1,)))
    pad = jnp.zeros((HALF, HALF), jnp.float32)
    r11 = s11 + eye - jnp.concatenate([mm(u10, u10, ((0,), (0,))), pad], axis=1)
    r21 = s21 - mm(u20, u10, ((0,), (0,)))
    w1 = factor(r11, row, lane)[:, HALF:]
    u21 = mm(w1, r21, ((1,), (1,)))
    gap = mm(u20, u20, ((0,), (0,))) + mm(u21, u21, ((0,), (0,)))
    r22 = s22 + eye - jnp.concatenate([gap, pad], axis=1)
    x10 = mm(u10, w0, ((0,), (0,)))
    w10 = -mm(w1, x10)
    x20 = mm(u20, w0, ((0,), (0,))) + mm(u21, w10, ((0,), (0,)))
    x21 = mm(u21, w1, ((0,), (0,)))
    w2 = factor(r22, row, lane)[:, HALF:]
    low_out = -mm(w2, jnp.concatenate([x20, x21], axis=1))
    for i in range(8):
        o_ref[i, 0:64] = jnp.concatenate([w0, w2], axis=1)
        o_ref[i, 64:128] = jnp.concatenate([w10, w1], axis=1)
        o_ref[i, 128:192] = low_out


def whiten(index, damp_exp, parts):
    smem = pl.BlockSpec(memory_space=pltpu.SMEM)
    return pl.pallas_call(
        whiten_kernel,
        in_specs=[smem, smem, WHOLE],
        out_specs=WHOLE,
        out_shape=pltpu.VMEM((8, OUT_ROWS, LANES), jnp.float32),
        compiler_params=params(8),
        name="whiten",
    )(index, damp_exp, on_chip(parts))


def spread_kernel(p_ref, o_ref):
    lane = lax.broadcasted_iota(jnp.int32, (HALF, LANES), 1)
    inside = lane < HALF
    for i in range(8):
        ends = p_ref[i, 0:64]
        o_ref[i, 0:64, 0:128] = jnp.where(inside, ends, 0.0)
        o_ref[i, 64:128, 0:128] = p_ref[i, 64:128]
        o_ref[i, 128:192, 0:128] = p_ref[i, 128:192]
        o_ref[i, 0:128, 128:192] = jnp.zeros((128, HALF), jnp.float32)
        o_ref[i, 128:192, 128:192] = rolled(ends, HALF)[:, :HALF]


def spread(packed):
    return pl.pallas_call(
        spread_kernel,
        grid=(1,),
        in_specs=[WHOLE],
        out_specs=pl.BlockSpec((8, HD, HD), lambda i: (0, 0, 0)),
        out_shape=jax.ShapeDtypeStruct((8, HD, HD), jnp.float32),
        compiler_params=params(8),
        name="spread",
    )(on_chip(packed))


def on_device(projected, weight_exp, damp_exp):
    dp, head = lax.axis_index("dp"), lax.axis_index("head")
    core = head % 2
    x, z, y_lo, y_hi = head // 4, dp % 4, dp // 4, head // 2 % 2
    y = 2 * y_hi + y_lo
    a = near(x) * 4 + near(y) * 2 + near(z)
    b = far(x) * 4 + far(y) * 2 + far(z)
    core, own_spot = core[None], jnp.where(core == 0, b, a)[None]
    theirs = [their_grams(projected, weight_exp, core, half) for half in range(2)]
    received = [lax.ppermute(part, DEVICES, partner_pairs()) for part in theirs]
    even = my_grams(projected, weight_exp, received[0], core, own_spot, 0).reshape(8, 4, ROWS, LANES)
    even = lax.all_to_all(even, DEVICES, 0, 0, tiled=True, axis_index_groups=cubes(0))
    odd = my_grams(projected, weight_exp, received[1], core, own_spot, 1)
    swapped = [odd[0]]
    for flip in range(1, 8):
        swapped.append(lax.ppermute(odd[flip], DEVICES, peers(flip)))
    even_sum = add_even(even)
    cube = add_odd(even_sum, swapped)
    parts = lax.all_to_all(cube, DEVICES, 0, 0, tiled=True, axis_index_groups=cubes(1))
    factors = whiten((head * 8 + dp)[None], damp_exp, parts)
    gathered = lax.all_to_all(factors, DEVICES, 0, 0, tiled=True, axis_index_groups=owner_groups())
    return spread(gathered)


def solution(mesh):
    return jax.shard_map(
        on_device,
        mesh=mesh,
        in_specs=(P(("dp", "head"), None), P(("dp", "head")), P()),
        out_specs=P("head", None, None),
        check_vma=False,
    )
```

```python
import jax
import jax.numpy as jnp
from jax import lax
from jax.experimental import pallas as pl
from jax.experimental.pallas import tpu as pltpu
from jax.sharding import PartitionSpec as P

HD = 192
HALF = 64
LANES = 128
ROWS = 152
BODY = 144
BLOCK_ROWS = 8 * BODY + 8
SLOT_ROWS = 4 * BODY + 8
TOKENS = 49152
PANEL = 2
DEVICES = ("dp", "head")


def place(device):
    dp, head = divmod(device, 16)
    y_lo, z = divmod(dp, 4)
    x, y_hi, core = head // 4, head // 2 % 2, head % 2
    return x, 2 * y_hi + y_lo, z, core


def near(v):
    return v >> 1


def far(v):
    return (v >> 1) ^ (v & 1)


def cubes(stage):
    groups = {}
    for device in range(128):
        x, y, z, core = place(device)
        inner = (near(x), near(y), near(z))
        outer = (far(x), far(y), far(z))
        key, member = (inner, outer) if (core == 0) == (stage == 0) else (outer, inner)
        first = member[0] if stage == 0 else member[0] ^ key[0]
        groups.setdefault((core, key), [0] * 8)[first * 4 + member[1] * 2 + member[2]] = device
    return [groups[k] for k in sorted(groups)]


def partner_pairs():
    return [(d, d ^ 1) for d in range(128)]


def peers(flip):
    pairs = []
    for group in cubes(0):
        pairs += [(group[i], group[i ^ flip]) for i in range(8)]
    return sorted(pairs)


def owner_groups():
    return [[dp * 16 + head for dp in range(8)] for head in range(16)]


def chunk_block(half, i):
    return (i >> 1) * 4 + half * 2 + (i & 1)


def spot(block, inner, core):
    x, y_hi = block >> 1, block & 1
    y_lo, z = inner >> 2, inner & 3
    y = 2 * y_hi + y_lo
    a, a_rest = near(x) * 4 + near(y) * 2 + near(z), near(y) * 2 + near(z)
    b, b_rest = far(x) * 4 + far(y) * 2 + far(z), far(y) * 2 + far(z)
    return jnp.where(core == 0, b, a), jnp.where(core == 0, a_rest, b_rest)


def on_chip(v):
    return pltpu.with_memory_space_constraint(v, pltpu.VMEM)


def off_chip(v):
    return pltpu.with_memory_space_constraint(v, pltpu.HBM)


WHOLE = pl.BlockSpec(memory_space=pltpu.VMEM)


def params(mebibytes, **kwargs):
    return pltpu.CompilerParams(vmem_limit_bytes=mebibytes << 20, **kwargs)


def rolled(v, by):
    return pltpu.roll(v, by, 1)


def block_grams(x_ref, w_ref, put, put_diag):
    w = w_ref[...]
    w3 = jnp.concatenate([w, w, w], axis=1)
    row = lax.broadcasted_iota(jnp.int32, (HALF, LANES), 0)
    lane = lax.broadcasted_iota(jnp.int32, (HALF, LANES), 1)
    row32, lane32 = row[:32], lane[:32]
    row16, lane16 = row[:16], lane[:16]
    contract = (((0,), (0,)), ((), ()))

    def finish(index, low, mid, first, last, at):
        put(index, 0, low)
        put(index, 64, jnp.where(lane - HALF > row, first, mid))

        def moved(v, to):
            return v if to == at else rolled(v, (to - at) % LANES)

        near_half = jnp.where(lane16 - 32 > row16, moved(last[:16], 32), moved(last[32:48], 0))
        far_half = jnp.where(lane16 - 96 > row16 + 16, moved(last[16:32], 96), moved(last[48:64], HALF))
        put(index, 128, jnp.where(lane16 < HALF, near_half, far_half))
        diag = jnp.sum(jnp.where(lane - HALF == row, first, 0.0), axis=0, keepdims=True)
        small = jnp.sum(jnp.where(lane32 - at == row32, last[:32], 0.0), axis=0, keepdims=True)
        diag = jnp.broadcast_to(diag, (8, LANES)) + moved(jnp.broadcast_to(small, (8, LANES)), 0)
        put_diag(index, diag[:1])

    for pair in range(4):
        x = x_ref[:, 384 * pair : 384 * (pair + 1)]
        xw = x * w3
        g = lax.dot_general(x[:, :256], xw[:, :256], contract, preferred_element_type=jnp.float32)
        f = lax.dot_general(x[:, 256:], xw[:, 128:], contract, preferred_element_type=jnp.float32)
        finish(2 * pair, g[128:192, :128], g[64:128, :128], rolled(g[:64, :128], HALF), g[128:192, 128:], 0)
        swapped = jnp.where(lane < HALF, f[64:, 128:], f[64:, :128])
        middle = jnp.where(lane < HALF, f[:64, 128:], f[:64, :128])
        finish(2 * pair + 1, rolled(swapped, HALF), rolled(middle, HALF), g[192:, 128:], f[64:, 128:], HALF)


def spread_weights(exp_ref, w_ref):
    for i in range(exp_ref.shape[0] // LANES):
        power = (1 << exp_ref[LANES * i : LANES * (i + 1)].reshape(1, LANES)).astype(jnp.float32)
        w_ref[LANES * i : LANES * (i + 1)] = jnp.broadcast_to(power, (LANES, LANES)).T.astype(jnp.bfloat16)


def their_grams_kernel(core_ref, x_ref, exp_ref, o_ref, w_ref):
    i = pl.program_id(0)

    @pl.when(i == 0)
    def _():
        spread_weights(exp_ref, w_ref)

    base = BLOCK_ROWS * i if o_ref.shape[0] > BLOCK_ROWS else 0

    def put(index, start, rows):
        o_ref[pl.ds(pl.multiple_of(base + BODY * index + start, 8), rows.shape[0])] = rows

    def put_diag(index, diag):
        o_ref[pl.ds(pl.multiple_of(base + 8 * BODY, 8) + index, 1)] = diag

    block_grams(x_ref, w_ref, put, put_diag)


def their_grams(projected, weight_exp, core, half):
    tokens = projected.shape[0]
    return pl.pallas_call(
        their_grams_kernel,
        grid_spec=pltpu.PrefetchScalarGridSpec(
            num_scalar_prefetch=1,
            grid=(4,),
            in_specs=[
                pl.BlockSpec((tokens, 8 * HD), lambda i, core: (0, 2 * chunk_block(half, i) + 1 - core[0])),
                pl.BlockSpec((tokens,), lambda i, core: (0,)),
            ],
            out_specs=WHOLE if half else pl.BlockSpec((BLOCK_ROWS, LANES), lambda i, core: (i, 0)),
            scratch_shapes=[pltpu.VMEM((tokens, LANES), jnp.bfloat16)],
        ),
        out_shape=(pltpu.VMEM if half else pltpu.HBM)((4 * BLOCK_ROWS, LANES), jnp.float32),
        compiler_params=params(12, dimension_semantics=("arbitrary",)),
        cost_estimate=pl.CostEstimate(flops=tokens * 64 * HD * HD, bytes_accessed=7_500_000, transcendentals=0),
        name="their_grams",
    )(core, off_chip(projected), off_chip(weight_exp))


def fill_slots(half, core_ref, x_ref, exp_ref, received_ref, all_ref, w_ref):
    i = pl.program_id(0)

    @pl.when(i == 0)
    def _():
        spread_weights(exp_ref, w_ref)
        for slot in range(8):
            all_ref[slot, SLOT_ROWS - 8 :] = jnp.zeros((8, LANES), jnp.float32)

    block = chunk_block(half, i)
    spots = [spot(block, inner, core_ref[0]) for inner in range(8)]

    def put(index, start, rows):
        slot, rest = spots[index]
        size = rows.shape[0]
        at = pl.multiple_of(BODY * rest + start, 8)
        all_ref[slot, pl.ds(at, size)] = rows + received_ref[BODY * index + start : BODY * index + start + size]

    def put_diag(index, diag):
        slot, rest = spots[index]
        all_ref[slot, pl.ds(4 * BODY + rest, 1)] = diag + received_ref[8 * BODY + index : 8 * BODY + index + 1]

    block_grams(x_ref, w_ref, put, put_diag)
    return spots


def my_even_kernel(core_ref, spot_ref, x_ref, exp_ref, received_ref, o_ref, w_ref, all_ref, sem):
    spots = fill_slots(0, core_ref, x_ref, exp_ref, received_ref, all_ref, w_ref)
    for slot, rest in spots:
        rows = pl.ds(pl.multiple_of(BODY * rest, 8), BODY)
        pltpu.make_async_copy(all_ref.at[slot, rows], o_ref.at[slot, rows], sem).start()

    @pl.when(pl.program_id(0) == pl.num_programs(0) - 1)
    def _():
        rows = pl.ds(4 * BODY, 8)
        pltpu.make_async_copy(all_ref.at[:, rows], o_ref.at[:, rows], sem).start()
        pltpu.make_async_copy(all_ref, o_ref, sem).wait()


def my_odd_kernel(core_ref, spot_ref, x_ref, exp_ref, received_ref, *refs):
    outs, (w_ref, all_ref) = refs[:8], refs[8:]
    fill_slots(1, core_ref, x_ref, exp_ref, received_ref, all_ref, w_ref)

    @pl.when(pl.program_id(0) == pl.num_programs(0) - 1)
    def _():
        for flip in range(8):
            outs[flip][...] = all_ref[spot_ref[0] ^ flip]


def my_grams(projected, weight_exp, received, core, own_spot, half):
    tokens = projected.shape[0]
    scratch = [pltpu.VMEM((tokens, LANES), jnp.bfloat16), pltpu.VMEM((8, SLOT_ROWS, LANES), jnp.float32)]
    if half:
        kernel, outs = my_odd_kernel, [WHOLE] * 8
        shapes = [pltpu.VMEM((SLOT_ROWS, LANES), jnp.float32)] * 8
    else:
        kernel, outs = my_even_kernel, pl.BlockSpec(memory_space=pl.ANY)
        shapes = pltpu.HBM((8, SLOT_ROWS, LANES), jnp.float32)
        scratch.append(pltpu.SemaphoreType.DMA(()))
    return pl.pallas_call(
        kernel,
        grid_spec=pltpu.PrefetchScalarGridSpec(
            num_scalar_prefetch=2,
            grid=(4,),
            in_specs=[
                pl.BlockSpec((tokens, 8 * HD), lambda i, core, spot: (0, 2 * chunk_block(half, i) + core[0])),
                pl.BlockSpec((tokens,), lambda i, core, spot: (0,)),
                pl.BlockSpec((BLOCK_ROWS, LANES), lambda i, core, spot: (i, 0)),
            ],
            out_specs=outs,
            scratch_shapes=scratch,
        ),
        out_shape=shapes,
        compiler_params=params(16, dimension_semantics=("arbitrary",)),
        cost_estimate=pl.CostEstimate(flops=tokens * 64 * HD * HD, bytes_accessed=10_000_000, transcendentals=0),
        name="my_grams",
    )(core, own_spot, off_chip(projected), off_chip(weight_exp), off_chip(received))


def even_kernel(even_ref, o_ref):
    def one(i, carry):
        rows = pl.ds(pl.multiple_of(8 * i, 8), 8)
        total = even_ref[0, rows]
        for k in range(1, 8):
            total = total + even_ref[k, rows]
        o_ref[rows] = total
        return carry

    lax.fori_loop(0, SLOT_ROWS // 8, one, 0, unroll=8)


def add_even(even):
    return pl.pallas_call(
        even_kernel,
        in_specs=[WHOLE],
        out_specs=WHOLE,
        out_shape=pltpu.VMEM((SLOT_ROWS, LANES), jnp.float32),
        compiler_params=params(8),
        cost_estimate=pl.CostEstimate(flops=6_000_000, bytes_accessed=3_000_000, transcendentals=0),
        name="add_even",
    )(off_chip(even))


def odd_kernel(even_ref, *refs):
    odd_refs, o_ref = refs[:8], refs[8]
    for i in range(4):
        rows = slice(BODY * i, BODY * (i + 1))
        o_ref[i, :BODY] = even_ref[rows]
        total = odd_refs[0][rows]
        for k in range(1, 8):
            total = total + odd_refs[k][rows]
        o_ref[4 + i, :BODY] = total
    last = slice(4 * BODY, SLOT_ROWS)
    total = odd_refs[0][last]
    for k in range(1, 8):
        total = total + odd_refs[k][last]
    for half, diags in enumerate((even_ref[last], total)):
        for i in range(4):
            o_ref[4 * half + i, BODY:] = jnp.broadcast_to(diags[i : i + 1], (8, LANES))


def add_odd(even_sum, odd):
    return pl.pallas_call(
        odd_kernel,
        in_specs=[WHOLE] * 9,
        out_specs=WHOLE,
        out_shape=pltpu.VMEM((8, ROWS, LANES), jnp.float32),
        compiler_params=params(8),
        name="add_odd",
    )(on_chip(even_sum), *[on_chip(v) for v in odd])


def mm(a, b, dims=((1,), (0,))):
    return lax.dot_general(a, b, (dims, ((), ())), precision=lax.Precision.HIGHEST, preferred_element_type=jnp.float32)


def factor(block, row, lane):
    m = jnp.where(lane - HALF == row, 1.0, block)
    tiles = [m[8 * t : 8 * t + 8] for t in range(8)]
    sub = lax.broadcasted_iota(jnp.int32, (8, LANES), 0)
    wide = lambda v: jnp.broadcast_to(v, (8, LANES))
    out = []
    for t in range(0, 8, PANEL):
        size = 8 * PANEL
        cols = {v: [wide(tiles[v][:, 8 * t + j : 8 * t + j + 1]) for j in range(size)] for v in range(t, 8)}
        q = []
        for j in range(size):
            own, k = t + j // 8, j % 8
            c, d = cols[own], tiles[own]
            r = 1.0 / c[j][k : k + 1]
            out.append(d[k : k + 1] * lax.rsqrt(c[j][k : k + 1]))
            q.append(wide(d[k : k + 1] * r))
            u = {l: wide(c[l][k : k + 1] * r) for l in range(j + 1, size)}
            for v in range(own, 8):
                part = jnp.where(sub > k, cols[v][j], 0.0) if v == own else cols[v][j]
                if v < t + PANEL:
                    tiles[v] = tiles[v] - part * q[j]
                for l in range(j + 1, size):
                    cols[v][l] = cols[v][l] - part * u[l]
        for v in range(t + PANEL, 8):
            for j in range(size):
                tiles[v] = tiles[v] - cols[v][j] * q[j]
    return jnp.concatenate(out, axis=0)


def whiten_kernel(index_ref, damp_ref, g_ref, o_ref):
    packed = g_ref[0]
    for i in range(1, 8):
        packed = packed + g_ref[i]
    packed = packed / TOKENS
    row = lax.broadcasted_iota(jnp.int32, (HALF, LANES), 0)
    lane = lax.broadcasted_iota(jnp.int32, (HALF, LANES), 1)
    row32, lane32 = row[:32], lane[:32]
    low = packed[0:64]
    mid = packed[64:128]
    tail = packed[128:144]
    extra = jnp.broadcast_to(packed[144:145], (HALF, LANES))
    turned = rolled(mid, HALF)
    inside = lane < HALF
    upper00 = jnp.where((lane > row) & inside, turned, 0.0)
    lower11 = jnp.where((lane < row), turned, 0.0)
    diag11 = jnp.where(lane == row, turned, 0.0)
    folded = jnp.concatenate([tail, rolled(tail, HALF)], axis=0)
    h10 = jnp.where(lane32 < 32, folded, 0.0)
    fturn = rolled(folded, LANES - 32)
    hup = jnp.where((lane32 > row32) & (lane32 < 32), fturn, 0.0)
    hlow = jnp.where(lane32 < row32, fturn, 0.0)
    hdiag = jnp.where(lane32 == row32, fturn, 0.0)
    extra_turned = rolled(extra, HALF)
    diag00 = jnp.where(lane == row, extra_turned, 0.0)
    hdiag0 = jnp.where(lane32 == row32, extra[:32], 0.0)
    lower22 = jnp.concatenate([jnp.zeros((32, LANES), jnp.float32), h10 + jnp.where(lane32 >= 32, rolled(hlow, 32), 0.0)], axis=0)
    upper22 = jnp.concatenate([hup, jnp.zeros((32, LANES), jnp.float32)], axis=0)
    diag22 = jnp.concatenate([hdiag0, rolled(hdiag, 32)], axis=0)

    def flip(v):
        return jnp.concatenate([v.T[:HALF], jnp.zeros((HALF, HALF), jnp.float32)], axis=1)

    s00 = upper00 + flip(upper00) + diag00
    s11 = lower11 + flip(lower11) + diag11
    off22 = lower22 + upper22
    s22 = off22 + flip(off22) + diag22
    trace = jnp.sum(jnp.sum(diag00 + diag11 + diag22, axis=0, keepdims=True), axis=1, keepdims=True)
    scale = (1 << damp_ref[index_ref[0]]).astype(jnp.float32)
    damping = (trace / HD + 1e-6) / scale
    eye = jnp.where(lane == row, jnp.broadcast_to(damping, (HALF, LANES)), 0.0)
    s10 = mid[:, :HALF]
    s20, s21 = low[:, :HALF], low[:, HALF:]

    w0 = factor(s00 + eye, row, lane)[:, HALF:]
    u10 = mm(w0, s10, ((1,), (1,)))
    u20 = mm(w0, s20, ((1,), (1,)))
    pad = jnp.zeros((HALF, HALF), jnp.float32)
    r11 = s11 + eye - jnp.concatenate([mm(u10, u10, ((0,), (0,))), pad], axis=1)
    r21 = s21 - mm(u20, u10, ((0,), (0,)))
    w1 = factor(r11, row, lane)[:, HALF:]
    u21 = mm(w1, r21, ((1,), (1,)))
    gap = mm(u20, u20, ((0,), (0,))) + mm(u21, u21, ((0,), (0,)))
    r22 = s22 + eye - jnp.concatenate([gap, pad], axis=1)
    x10 = mm(u10, w0, ((0,), (0,)))
    w10 = -mm(w1, x10)
    x20 = mm(u20, w0, ((0,), (0,))) + mm(u21, w10, ((0,), (0,)))
    x21 = mm(u21, w1, ((0,), (0,)))
    w2 = factor(r22, row, lane)[:, HALF:]
    low_out = -mm(w2, jnp.concatenate([x20, x21], axis=1))

    def twice(v):
        return jnp.concatenate([v, v], axis=1)

    turned0 = twice(w0).T
    turned0 = jnp.concatenate([turned0[:HALF], turned0[HALF:]], axis=1)
    middle = jnp.where(lane - HALF > row, turned0, jnp.concatenate([w10, w1], axis=1))
    w2_wide = twice(w2)
    corner = w2_wide[:32]
    corner = jnp.concatenate([corner] * 4, axis=0).T[:32]
    tri = jnp.where((lane32 & 63) - 32 > row32, corner, w2_wide[32:])
    tri = jnp.where(lane[:16] < HALF, tri[:16], tri[16:])
    diag = jnp.sum(jnp.where(lane == row, twice(w0), 0.0), axis=0, keepdims=True)
    diag += jnp.sum(jnp.where(lane32 - HALF == row32, w2_wide[:32], 0.0), axis=0, keepdims=True)
    for i in range(8):
        o_ref[i, 0:64] = low_out
        o_ref[i, 64:128] = middle
        o_ref[i, 128:144] = tri
        o_ref[i, 144:152] = jnp.broadcast_to(diag, (8, LANES))


def whiten(index, damp_exp, parts):
    smem = pl.BlockSpec(memory_space=pltpu.SMEM)
    return pl.pallas_call(
        whiten_kernel,
        in_specs=[smem, smem, WHOLE],
        out_specs=WHOLE,
        out_shape=pltpu.VMEM((8, ROWS, LANES), jnp.float32),
        compiler_params=params(8),
        name="whiten",
    )(index, damp_exp, on_chip(parts))


def spread_kernel(p_ref, o_ref):
    row = lax.broadcasted_iota(jnp.int32, (HALF, LANES), 0)
    lane = lax.broadcasted_iota(jnp.int32, (HALF, LANES), 1)
    row32, lane32 = row[:32], lane[:32]
    for i in range(8):
        middle = p_ref[i, 64:128]
        tail = p_ref[i, 128:144]
        diag = p_ref[i, 144:145]
        turned = jnp.concatenate([middle, middle], axis=0).T[HALF:]
        first = jnp.where(lane < row, turned, jnp.where(lane == row, diag, 0.0))
        o_ref[i, 0:64, 0:128] = first
        o_ref[i, 64:128, 0:128] = jnp.where(lane - HALF <= row, middle, 0.0)
        o_ref[i, 128:192, 0:128] = p_ref[i, 0:64]
        o_ref[i, 0:128, 128:192] = jnp.zeros((128, HALF), jnp.float32)
        lower = jnp.concatenate([tail, rolled(tail, HALF)], axis=0)
        corner = jnp.concatenate([lower] * 4, axis=0).T[32:64]
        corner_diag = rolled(jnp.broadcast_to(diag, (32, LANES)), HALF)
        top = jnp.where(lane32 < row32, corner, jnp.where(lane32 == row32, corner_diag, 0.0))
        bottom = jnp.where(lane32 - 32 <= row32, lower, 0.0)
        o_ref[i, 128:160, 128:192] = top[:, :HALF]
        o_ref[i, 160:192, 128:192] = bottom[:, :HALF]


def spread(packed):
    return pl.pallas_call(
        spread_kernel,
        grid=(1,),
        in_specs=[WHOLE],
        out_specs=pl.BlockSpec((8, HD, HD), lambda i: (0, 0, 0)),
        out_shape=jax.ShapeDtypeStruct((8, HD, HD), jnp.float32),
        compiler_params=params(8),
        name="spread",
    )(on_chip(packed))


def on_device(projected, weight_exp, damp_exp):
    dp, head = lax.axis_index("dp"), lax.axis_index("head")
    core = head % 2
    x, z, y_lo, y_hi = head // 4, dp % 4, dp // 4, head // 2 % 2
    y = 2 * y_hi + y_lo
    a = near(x) * 4 + near(y) * 2 + near(z)
    b = far(x) * 4 + far(y) * 2 + far(z)
    core, own_spot = core[None], jnp.where(core == 0, b, a)[None]
    theirs = [their_grams(projected, weight_exp, core, half) for half in range(2)]
    received = [lax.ppermute(part, DEVICES, partner_pairs()) for part in theirs]
    even = my_grams(projected, weight_exp, received[0], core, own_spot, 0)
    even = lax.all_to_all(even, DEVICES, 0, 0, tiled=True, axis_index_groups=cubes(0))
    odd = my_grams(projected, weight_exp, received[1], core, own_spot, 1)
    swapped = [odd[0]]
    for flip in range(1, 8):
        swapped.append(lax.ppermute(odd[flip], DEVICES, peers(flip)))
    even_sum = add_even(even)
    cube = add_odd(even_sum, swapped)
    parts = lax.all_to_all(cube, DEVICES, 0, 0, tiled=True, axis_index_groups=cubes(1))
    factors = whiten((head * 8 + dp)[None], damp_exp, parts)
    gathered = lax.all_to_all(factors, DEVICES, 0, 0, tiled=True, axis_index_groups=owner_groups())
    return spread(gathered)


def solution(mesh):
    return jax.shard_map(
        on_device,
        mesh=mesh,
        in_specs=(P(("dp", "head"), None), P(("dp", "head")), P()),
        out_specs=P("head", None, None),
        check_vma=False,
    )
```

```python
import jax
import jax.numpy as jnp
from jax import lax
from jax.experimental import pallas as pl
from jax.experimental.pallas import tpu as pltpu
from jax.sharding import PartitionSpec as P

HD = 192
HALF = 64
LANES = 128
ROWS = 152
BODY = 144
BLOCK_ROWS = 8 * BODY + 8
SLOT_ROWS = 4 * BODY + 8
TOKENS = 49152
PANEL = 2
DEVICES = ("dp", "head")


def place(device):
    dp, head = divmod(device, 16)
    y_lo, z = divmod(dp, 4)
    x, y_hi, core = head // 4, head // 2 % 2, head % 2
    return x, 2 * y_hi + y_lo, z, core


def near(v):
    return v >> 1


def far(v):
    return (v >> 1) ^ (v & 1)


def cubes(stage):
    groups = {}
    for device in range(128):
        x, y, z, core = place(device)
        inner = (near(x), near(y), near(z))
        outer = (far(x), far(y), far(z))
        key, member = (inner, outer) if (core == 0) == (stage == 0) else (outer, inner)
        first = member[0] if stage == 0 else member[0] ^ key[0]
        groups.setdefault((core, key), [0] * 8)[first * 4 + member[1] * 2 + member[2]] = device
    return [groups[k] for k in sorted(groups)]


def partner_pairs():
    return [(d, d ^ 1) for d in range(128)]


def peers(flip):
    pairs = []
    for group in cubes(0):
        pairs += [(group[i], group[i ^ flip]) for i in range(8)]
    return sorted(pairs)


def owner_groups():
    return [[dp * 16 + head for dp in range(8)] for head in range(16)]


def chunk_block(half, i):
    return (i >> 1) * 4 + half * 2 + (i & 1)


def spot(block, inner, core):
    x, y_hi = block >> 1, block & 1
    y_lo, z = inner >> 2, inner & 3
    y = 2 * y_hi + y_lo
    a, a_rest = near(x) * 4 + near(y) * 2 + near(z), near(y) * 2 + near(z)
    b, b_rest = far(x) * 4 + far(y) * 2 + far(z), far(y) * 2 + far(z)
    return jnp.where(core == 0, b, a), jnp.where(core == 0, a_rest, b_rest)


def on_chip(v):
    return pltpu.with_memory_space_constraint(v, pltpu.VMEM)


def off_chip(v):
    return pltpu.with_memory_space_constraint(v, pltpu.HBM)


WHOLE = pl.BlockSpec(memory_space=pltpu.VMEM)


def params(mebibytes, **kwargs):
    return pltpu.CompilerParams(vmem_limit_bytes=mebibytes << 20, **kwargs)


def rolled(v, by):
    return pltpu.roll(v, by, 1)


def block_grams(x_ref, w_ref, put, put_diag):
    w = w_ref[...]
    w3 = jnp.concatenate([w, w, w], axis=1)
    row = lax.broadcasted_iota(jnp.int32, (HALF, LANES), 0)
    lane = lax.broadcasted_iota(jnp.int32, (HALF, LANES), 1)
    row32, lane32 = row[:32], lane[:32]
    row16, lane16 = row[:16], lane[:16]
    contract = (((0,), (0,)), ((), ()))

    def finish(index, low, mid, first, last, at):
        put(index, 0, low)
        put(index, 64, jnp.where(lane - HALF > row, first, mid))

        def moved(v, to):
            return v if to == at else rolled(v, (to - at) % LANES)

        near_half = jnp.where(lane16 - 32 > row16, moved(last[:16], 32), moved(last[32:48], 0))
        far_half = jnp.where(lane16 - 96 > row16 + 16, moved(last[16:32], 96), moved(last[48:64], HALF))
        put(index, 128, jnp.where(lane16 < HALF, near_half, far_half))
        diag = jnp.sum(jnp.where(lane - HALF == row, first, 0.0), axis=0, keepdims=True)
        small = jnp.sum(jnp.where(lane32 - at == row32, last[:32], 0.0), axis=0, keepdims=True)
        diag = jnp.broadcast_to(diag, (8, LANES)) + moved(jnp.broadcast_to(small, (8, LANES)), 0)
        put_diag(index, diag[:1])

    for pair in range(4):
        x = x_ref[:, 384 * pair : 384 * (pair + 1)]
        xw = x * w3
        g = lax.dot_general(x[:, :256], xw[:, :256], contract, preferred_element_type=jnp.float32)
        f = lax.dot_general(x[:, 256:], xw[:, 128:], contract, preferred_element_type=jnp.float32)
        finish(2 * pair, g[128:192, :128], g[64:128, :128], rolled(g[:64, :128], HALF), g[128:192, 128:], 0)
        swapped = jnp.where(lane < HALF, f[64:, 128:], f[64:, :128])
        middle = jnp.where(lane < HALF, f[:64, 128:], f[:64, :128])
        finish(2 * pair + 1, rolled(swapped, HALF), rolled(middle, HALF), g[192:, 128:], f[64:, 128:], HALF)


def spread_weights(exp_ref, w_ref):
    for i in range(exp_ref.shape[0] // LANES):
        power = (1 << exp_ref[LANES * i : LANES * (i + 1)].reshape(1, LANES)).astype(jnp.float32)
        w_ref[LANES * i : LANES * (i + 1)] = jnp.broadcast_to(power, (LANES, LANES)).T.astype(jnp.bfloat16)


def their_grams_kernel(core_ref, xa_ref, xb_ref, exp_ref, o_ref, w_ref):
    i = pl.program_id(0)

    @pl.when(i == 0)
    def _():
        spread_weights(exp_ref, w_ref)

    for part, x_ref in enumerate((xa_ref, xb_ref)):
        base = BLOCK_ROWS * (2 * i + part) if o_ref.shape[0] > 2 * BLOCK_ROWS else BLOCK_ROWS * part

        def put(index, start, rows, base=base):
            o_ref[pl.ds(pl.multiple_of(base + BODY * index + start, 8), rows.shape[0])] = rows

        def put_diag(index, diag, base=base):
            o_ref[pl.ds(pl.multiple_of(base + 8 * BODY, 8) + index, 1)] = diag

        block_grams(x_ref, w_ref, put, put_diag)


def their_grams(projected, weight_exp, core, half):
    tokens = projected.shape[0]
    x_spec = lambda part: pl.BlockSpec(
        (tokens, 8 * HD), lambda i, core: (0, 2 * chunk_block(half, 2 * i + part) + 1 - core[0])
    )
    return pl.pallas_call(
        their_grams_kernel,
        grid_spec=pltpu.PrefetchScalarGridSpec(
            num_scalar_prefetch=1,
            grid=(2,),
            in_specs=[x_spec(0), x_spec(1), pl.BlockSpec((tokens,), lambda i, core: (0,))],
            out_specs=pl.BlockSpec((2 * BLOCK_ROWS, LANES), lambda i, core: (i, 0)) if half else WHOLE,
            scratch_shapes=[pltpu.VMEM((tokens, LANES), jnp.bfloat16)],
        ),
        out_shape=(pltpu.HBM if half else pltpu.VMEM)((4 * BLOCK_ROWS, LANES), jnp.float32),
        compiler_params=params(16, dimension_semantics=("arbitrary",)),
        cost_estimate=pl.CostEstimate(flops=tokens * 64 * HD * HD, bytes_accessed=7_500_000, transcendentals=0),
        name="their_grams",
    )(core, off_chip(projected), off_chip(projected), off_chip(weight_exp))


def fill_slots(half, core_ref, x_refs, exp_ref, received_ref, all_ref, w_ref):
    i = pl.program_id(0)

    @pl.when(i == 0)
    def _():
        spread_weights(exp_ref, w_ref)
        for slot in range(8):
            all_ref[slot, SLOT_ROWS - 8 :] = jnp.zeros((8, LANES), jnp.float32)

    spots = []
    for part, x_ref in enumerate(x_refs):
        spots.append([spot(chunk_block(half, 2 * i + part), inner, core_ref[0]) for inner in range(8)])

        def put(index, start, rows, part=part):
            slot, rest = spots[part][index]
            at = pl.ds(pl.multiple_of(BODY * rest + start, 8), rows.shape[0])
            source = BLOCK_ROWS * part + BODY * index + start
            all_ref[slot, at] = rows + received_ref[source : source + rows.shape[0]]

        def put_diag(index, diag, part=part):
            slot, rest = spots[part][index]
            source = BLOCK_ROWS * part + 8 * BODY + index
            all_ref[slot, pl.ds(4 * BODY + rest, 1)] = diag + received_ref[source : source + 1]

        block_grams(x_ref, w_ref, put, put_diag)
    return spots[0] + spots[1]


def my_even_kernel(core_ref, spot_ref, xa_ref, xb_ref, exp_ref, received_ref, o_ref, w_ref, all_ref, sem):
    spots = fill_slots(0, core_ref, (xa_ref, xb_ref), exp_ref, received_ref, all_ref, w_ref)
    for slot, rest in spots:
        rows = pl.ds(pl.multiple_of(BODY * rest, 8), BODY)
        pltpu.make_async_copy(all_ref.at[slot, rows], o_ref.at[slot, rows], sem).start()

    @pl.when(pl.program_id(0) == pl.num_programs(0) - 1)
    def _():
        rows = pl.ds(4 * BODY, 8)
        pltpu.make_async_copy(all_ref.at[:, rows], o_ref.at[:, rows], sem).start()
        pltpu.make_async_copy(all_ref, o_ref, sem).wait()


def my_odd_kernel(core_ref, spot_ref, xa_ref, xb_ref, exp_ref, received_ref, *refs):
    outs, (w_ref, all_ref) = refs[:8], refs[8:]
    fill_slots(1, core_ref, (xa_ref, xb_ref), exp_ref, received_ref, all_ref, w_ref)

    @pl.when(pl.program_id(0) == pl.num_programs(0) - 1)
    def _():
        for flip in range(8):
            outs[flip][...] = all_ref[spot_ref[0] ^ flip]


def my_grams(projected, weight_exp, received, core, own_spot, half):
    tokens = projected.shape[0]
    scratch = [pltpu.VMEM((tokens, LANES), jnp.bfloat16), pltpu.VMEM((8, SLOT_ROWS, LANES), jnp.float32)]
    if half:
        kernel, outs = my_odd_kernel, [WHOLE] * 8
        shapes = [pltpu.VMEM((SLOT_ROWS, LANES), jnp.float32)] * 8
    else:
        kernel, outs = my_even_kernel, pl.BlockSpec(memory_space=pl.ANY)
        shapes = pltpu.HBM((8, SLOT_ROWS, LANES), jnp.float32)
        scratch.append(pltpu.SemaphoreType.DMA(()))
    x_spec = lambda part: pl.BlockSpec(
        (tokens, 8 * HD), lambda i, core, spot: (0, 2 * chunk_block(half, 2 * i + part) + core[0])
    )
    return pl.pallas_call(
        kernel,
        grid_spec=pltpu.PrefetchScalarGridSpec(
            num_scalar_prefetch=2,
            grid=(2,),
            in_specs=[
                x_spec(0),
                x_spec(1),
                pl.BlockSpec((tokens,), lambda i, core, spot: (0,)),
                pl.BlockSpec((2 * BLOCK_ROWS, LANES), lambda i, core, spot: (i, 0)),
            ],
            out_specs=outs,
            scratch_shapes=scratch,
        ),
        out_shape=shapes,
        compiler_params=params(20, dimension_semantics=("arbitrary",)),
        cost_estimate=pl.CostEstimate(flops=tokens * 64 * HD * HD, bytes_accessed=10_000_000, transcendentals=0),
        name="my_grams",
    )(core, own_spot, off_chip(projected), off_chip(projected), off_chip(weight_exp), off_chip(received))


def even_kernel(even_ref, o_ref):
    def one(i, carry):
        rows = pl.ds(pl.multiple_of(8 * i, 8), 8)
        total = even_ref[0, rows]
        for k in range(1, 8):
            total = total + even_ref[k, rows]
        o_ref[rows] = total
        return carry

    lax.fori_loop(0, SLOT_ROWS // 8, one, 0, unroll=8)


def add_even(even):
    return pl.pallas_call(
        even_kernel,
        in_specs=[WHOLE],
        out_specs=WHOLE,
        out_shape=pltpu.VMEM((SLOT_ROWS, LANES), jnp.float32),
        compiler_params=params(8),
        cost_estimate=pl.CostEstimate(flops=6_000_000, bytes_accessed=3_000_000, transcendentals=0),
        name="add_even",
    )(off_chip(even))


def odd_kernel(even_ref, *refs):
    odd_refs, o_ref = refs[:8], refs[8]
    for i in range(4):
        rows = slice(BODY * i, BODY * (i + 1))
        o_ref[i, :BODY] = even_ref[rows]
        total = odd_refs[0][rows]
        for k in range(1, 8):
            total = total + odd_refs[k][rows]
        o_ref[4 + i, :BODY] = total
    last = slice(4 * BODY, SLOT_ROWS)
    total = odd_refs[0][last]
    for k in range(1, 8):
        total = total + odd_refs[k][last]
    for half, diags in enumerate((even_ref[last], total)):
        for i in range(4):
            o_ref[4 * half + i, BODY:] = jnp.broadcast_to(diags[i : i + 1], (8, LANES))


def add_odd(even_sum, odd):
    return pl.pallas_call(
        odd_kernel,
        in_specs=[WHOLE] * 9,
        out_specs=WHOLE,
        out_shape=pltpu.VMEM((8, ROWS, LANES), jnp.float32),
        compiler_params=params(8),
        name="add_odd",
    )(on_chip(even_sum), *[on_chip(v) for v in odd])


def mm(a, b, dims=((1,), (0,))):
    return lax.dot_general(a, b, (dims, ((), ())), precision=lax.Precision.HIGHEST, preferred_element_type=jnp.float32)


def factor(block, row, lane):
    m = jnp.where(lane - HALF == row, 1.0, block)
    tiles = [m[8 * t : 8 * t + 8] for t in range(8)]
    sub = lax.broadcasted_iota(jnp.int32, (8, LANES), 0)
    wide = lambda v: jnp.broadcast_to(v, (8, LANES))
    out = []
    for t in range(0, 8, PANEL):
        size = 8 * PANEL
        cols = {v: [wide(tiles[v][:, 8 * t + j : 8 * t + j + 1]) for j in range(size)] for v in range(t, 8)}
        q = []
        for j in range(size):
            own, k = t + j // 8, j % 8
            c, d = cols[own], tiles[own]
            r = 1.0 / c[j][k : k + 1]
            out.append(d[k : k + 1] * lax.rsqrt(c[j][k : k + 1]))
            q.append(wide(d[k : k + 1] * r))
            u = {l: wide(c[l][k : k + 1] * r) for l in range(j + 1, size)}
            for v in range(own, 8):
                part = jnp.where(sub > k, cols[v][j], 0.0) if v == own else cols[v][j]
                if v < t + PANEL:
                    tiles[v] = tiles[v] - part * q[j]
                for l in range(j + 1, size):
                    cols[v][l] = cols[v][l] - part * u[l]
        for v in range(t + PANEL, 8):
            for j in range(size):
                tiles[v] = tiles[v] - cols[v][j] * q[j]
    return jnp.concatenate(out, axis=0)


def whiten_kernel(index_ref, damp_ref, g_ref, o_ref):
    packed = g_ref[0]
    for i in range(1, 8):
        packed = packed + g_ref[i]
    packed = packed / TOKENS
    row = lax.broadcasted_iota(jnp.int32, (HALF, LANES), 0)
    lane = lax.broadcasted_iota(jnp.int32, (HALF, LANES), 1)
    row32, lane32 = row[:32], lane[:32]
    low = packed[0:64]
    mid = packed[64:128]
    tail = packed[128:144]
    extra = jnp.broadcast_to(packed[144:145], (HALF, LANES))
    turned = rolled(mid, HALF)
    inside = lane < HALF
    upper00 = jnp.where((lane > row) & inside, turned, 0.0)
    lower11 = jnp.where((lane < row), turned, 0.0)
    diag11 = jnp.where(lane == row, turned, 0.0)
    folded = jnp.concatenate([tail, rolled(tail, HALF)], axis=0)
    h10 = jnp.where(lane32 < 32, folded, 0.0)
    fturn = rolled(folded, LANES - 32)
    hup = jnp.where((lane32 > row32) & (lane32 < 32), fturn, 0.0)
    hlow = jnp.where(lane32 < row32, fturn, 0.0)
    hdiag = jnp.where(lane32 == row32, fturn, 0.0)
    extra_turned = rolled(extra, HALF)
    diag00 = jnp.where(lane == row, extra_turned, 0.0)
    hdiag0 = jnp.where(lane32 == row32, extra[:32], 0.0)
    lower22 = jnp.concatenate([jnp.zeros((32, LANES), jnp.float32), h10 + jnp.where(lane32 >= 32, rolled(hlow, 32), 0.0)], axis=0)
    upper22 = jnp.concatenate([hup, jnp.zeros((32, LANES), jnp.float32)], axis=0)
    diag22 = jnp.concatenate([hdiag0, rolled(hdiag, 32)], axis=0)

    def flip(v):
        return jnp.concatenate([v.T[:HALF], jnp.zeros((HALF, HALF), jnp.float32)], axis=1)

    s00 = upper00 + flip(upper00) + diag00
    s11 = lower11 + flip(lower11) + diag11
    off22 = lower22 + upper22
    s22 = off22 + flip(off22) + diag22
    trace = jnp.sum(jnp.sum(diag00 + diag11 + diag22, axis=0, keepdims=True), axis=1, keepdims=True)
    scale = (1 << damp_ref[index_ref[0]]).astype(jnp.float32)
    damping = (trace / HD + 1e-6) / scale
    eye = jnp.where(lane == row, jnp.broadcast_to(damping, (HALF, LANES)), 0.0)
    s10 = mid[:, :HALF]
    s20, s21 = low[:, :HALF], low[:, HALF:]

    w0 = factor(s00 + eye, row, lane)[:, HALF:]
    u10 = mm(w0, s10, ((1,), (1,)))
    u20 = mm(w0, s20, ((1,), (1,)))
    pad = jnp.zeros((HALF, HALF), jnp.float32)
    r11 = s11 + eye - jnp.concatenate([mm(u10, u10, ((0,), (0,))), pad], axis=1)
    r21 = s21 - mm(u20, u10, ((0,), (0,)))
    w1 = factor(r11, row, lane)[:, HALF:]
    u21 = mm(w1, r21, ((1,), (1,)))
    gap = mm(u20, u20, ((0,), (0,))) + mm(u21, u21, ((0,), (0,)))
    r22 = s22 + eye - jnp.concatenate([gap, pad], axis=1)
    x10 = mm(u10, w0, ((0,), (0,)))
    w10 = -mm(w1, x10)
    x20 = mm(u20, w0, ((0,), (0,))) + mm(u21, w10, ((0,), (0,)))
    x21 = mm(u21, w1, ((0,), (0,)))
    w2 = factor(r22, row, lane)[:, HALF:]
    low_out = -mm(w2, jnp.concatenate([x20, x21], axis=1))

    def twice(v):
        return jnp.concatenate([v, v], axis=1)

    turned0 = twice(w0).T
    turned0 = jnp.concatenate([turned0[:HALF], turned0[HALF:]], axis=1)
    middle = jnp.where(lane - HALF > row, turned0, jnp.concatenate([w10, w1], axis=1))
    w2_wide = twice(w2)
    corner = w2_wide[:32]
    corner = jnp.concatenate([corner] * 4, axis=0).T[:32]
    tri = jnp.where((lane32 & 63) - 32 > row32, corner, w2_wide[32:])
    tri = jnp.where(lane[:16] < HALF, tri[:16], tri[16:])
    diag = jnp.sum(jnp.where(lane == row, twice(w0), 0.0), axis=0, keepdims=True)
    diag += jnp.sum(jnp.where(lane32 - HALF == row32, w2_wide[:32], 0.0), axis=0, keepdims=True)
    for i in range(8):
        o_ref[i, 0:64] = low_out
        o_ref[i, 64:128] = middle
        o_ref[i, 128:144] = tri
        o_ref[i, 144:152] = jnp.broadcast_to(diag, (8, LANES))


def whiten(index, damp_exp, parts):
    smem = pl.BlockSpec(memory_space=pltpu.SMEM)
    return pl.pallas_call(
        whiten_kernel,
        in_specs=[smem, smem, WHOLE],
        out_specs=WHOLE,
        out_shape=pltpu.VMEM((8, ROWS, LANES), jnp.float32),
        compiler_params=params(8),
        name="whiten",
    )(index, damp_exp, on_chip(parts))


def spread_kernel(p_ref, o_ref):
    row = lax.broadcasted_iota(jnp.int32, (HALF, LANES), 0)
    lane = lax.broadcasted_iota(jnp.int32, (HALF, LANES), 1)
    row32, lane32 = row[:32], lane[:32]
    first_matrix = o_ref.shape[0] * pl.program_id(0)
    for i in range(o_ref.shape[0]):
        middle = p_ref[first_matrix + i, 64:128]
        tail = p_ref[first_matrix + i, 128:144]
        diag = p_ref[first_matrix + i, 144:145]
        turned = jnp.concatenate([middle, middle], axis=0).T[HALF:]
        first = jnp.where(lane < row, turned, jnp.where(lane == row, diag, 0.0))
        o_ref[i, 0:64, 0:128] = first
        o_ref[i, 64:128, 0:128] = jnp.where(lane - HALF <= row, middle, 0.0)
        o_ref[i, 128:192, 0:128] = p_ref[first_matrix + i, 0:64]
        o_ref[i, 0:128, 128:192] = jnp.zeros((128, HALF), jnp.float32)
        lower = jnp.concatenate([tail, rolled(tail, HALF)], axis=0)
        corner = jnp.concatenate([lower] * 4, axis=0).T[32:64]
        corner_diag = rolled(jnp.broadcast_to(diag, (32, LANES)), HALF)
        top = jnp.where(lane32 < row32, corner, jnp.where(lane32 == row32, corner_diag, 0.0))
        bottom = jnp.where(lane32 - 32 <= row32, lower, 0.0)
        o_ref[i, 128:160, 128:192] = top[:, :HALF]
        o_ref[i, 160:192, 128:192] = bottom[:, :HALF]


def spread(packed):
    return pl.pallas_call(
        spread_kernel,
        grid=(2,),
        in_specs=[WHOLE],
        out_specs=pl.BlockSpec((4, HD, HD), lambda i: (i, 0, 0)),
        out_shape=jax.ShapeDtypeStruct((8, HD, HD), jnp.float32),
        compiler_params=params(8),
        name="spread",
    )(on_chip(packed))


def on_device(projected, weight_exp, damp_exp):
    dp, head = lax.axis_index("dp"), lax.axis_index("head")
    core = head % 2
    x, z, y_lo, y_hi = head // 4, dp % 4, dp // 4, head // 2 % 2
    y = 2 * y_hi + y_lo
    a = near(x) * 4 + near(y) * 2 + near(z)
    b = far(x) * 4 + far(y) * 2 + far(z)
    core, own_spot = core[None], jnp.where(core == 0, b, a)[None]
    theirs = [their_grams(projected, weight_exp, core, half) for half in range(2)]
    received = [lax.ppermute(part, DEVICES, partner_pairs()) for part in theirs]
    even = my_grams(projected, weight_exp, received[0], core, own_spot, 0)
    even = lax.all_to_all(even, DEVICES, 0, 0, tiled=True, axis_index_groups=cubes(0))
    odd = my_grams(projected, weight_exp, received[1], core, own_spot, 1)
    swapped = [odd[0]]
    for flip in range(1, 8):
        swapped.append(lax.ppermute(odd[flip], DEVICES, peers(flip)))
    even_sum = add_even(even)
    cube = add_odd(even_sum, swapped)
    parts = lax.all_to_all(cube, DEVICES, 0, 0, tiled=True, axis_index_groups=cubes(1))
    factors = whiten((head * 8 + dp)[None], damp_exp, parts)
    gathered = lax.all_to_all(factors, DEVICES, 0, 0, tiled=True, axis_index_groups=owner_groups())
    return spread(gathered)


def solution(mesh):
    return jax.shard_map(
        on_device,
        mesh=mesh,
        in_specs=(P(("dp", "head"), None), P(("dp", "head")), P()),
        out_specs=P("head", None, None),
        check_vma=False,
    )
```

```python
import jax
import jax.numpy as jnp
from jax import lax
from jax.experimental import pallas as pl
from jax.experimental.pallas import tpu as pltpu
from jax.sharding import PartitionSpec as P

HD = 192
HALF = 64
LANES = 128
ROWS = 152
BODY = 144
BLOCK_ROWS = 8 * BODY + 8
SLOT_ROWS = 4 * BODY + 8
TOKENS = 49152
PANEL = 2
DEVICES = ("dp", "head")


def place(device):
    dp, head = divmod(device, 16)
    y_lo, z = divmod(dp, 4)
    x, y_hi, core = head // 4, head // 2 % 2, head % 2
    return x, 2 * y_hi + y_lo, z, core


def near(v):
    return v >> 1


def far(v):
    return (v >> 1) ^ (v & 1)


def cubes(stage):
    groups = {}
    for device in range(128):
        x, y, z, core = place(device)
        inner = (near(x), near(y), near(z))
        outer = (far(x), far(y), far(z))
        key, member = (inner, outer) if (core == 0) == (stage == 0) else (outer, inner)
        first = member[0] if stage == 0 else member[0] ^ key[0]
        groups.setdefault((core, key), [0] * 8)[first * 4 + member[1] * 2 + member[2]] = device
    return [groups[k] for k in sorted(groups)]


def partner_pairs():
    return [(d, d ^ 1) for d in range(128)]


def peers(flip):
    pairs = []
    for group in cubes(0):
        pairs += [(group[i], group[i ^ flip]) for i in range(8)]
    return sorted(pairs)


def owner_groups():
    return [[dp * 16 + head for dp in range(8)] for head in range(16)]


def chunk_block(half, i):
    return (i >> 1) * 4 + half * 2 + (i & 1)


def spot(block, inner, core):
    x, y_hi = block >> 1, block & 1
    y_lo, z = inner >> 2, inner & 3
    y = 2 * y_hi + y_lo
    a, a_rest = near(x) * 4 + near(y) * 2 + near(z), near(y) * 2 + near(z)
    b, b_rest = far(x) * 4 + far(y) * 2 + far(z), far(y) * 2 + far(z)
    return jnp.where(core == 0, b, a), jnp.where(core == 0, a_rest, b_rest)


def on_chip(v):
    return pltpu.with_memory_space_constraint(v, pltpu.VMEM)


def off_chip(v):
    return pltpu.with_memory_space_constraint(v, pltpu.HBM)


WHOLE = pl.BlockSpec(memory_space=pltpu.VMEM)


def params(mebibytes, **kwargs):
    return pltpu.CompilerParams(vmem_limit_bytes=mebibytes << 20, **kwargs)


def rolled(v, by):
    return pltpu.roll(v, by, 1)


def block_grams(x_ref, w_ref, put, put_diag):
    w = w_ref[...]
    w3 = jnp.concatenate([w, w, w], axis=1)
    row = lax.broadcasted_iota(jnp.int32, (HALF, LANES), 0)
    lane = lax.broadcasted_iota(jnp.int32, (HALF, LANES), 1)
    row32, lane32 = row[:32], lane[:32]
    row16, lane16 = row[:16], lane[:16]
    contract = (((0,), (0,)), ((), ()))

    def finish(index, low, mid, first, last, at):
        put(index, 0, low)
        put(index, 64, jnp.where(lane - HALF > row, first, mid))

        def moved(v, to):
            return v if to == at else rolled(v, (to - at) % LANES)

        near_half = jnp.where(lane16 - 32 > row16, moved(last[:16], 32), moved(last[32:48], 0))
        far_half = jnp.where(lane16 - 96 > row16 + 16, moved(last[16:32], 96), moved(last[48:64], HALF))
        put(index, 128, jnp.where(lane16 < HALF, near_half, far_half))
        diag = jnp.sum(jnp.where(lane - HALF == row, first, 0.0), axis=0, keepdims=True)
        small = jnp.sum(jnp.where(lane32 - at == row32, last[:32], 0.0), axis=0, keepdims=True)
        diag = jnp.broadcast_to(diag, (8, LANES)) + moved(jnp.broadcast_to(small, (8, LANES)), 0)
        put_diag(index, diag[:1])

    for pair in range(4):
        x = x_ref[:, 384 * pair : 384 * (pair + 1)]
        xw = x * w3
        g = lax.dot_general(x[:, :256], xw[:, :256], contract, preferred_element_type=jnp.float32)
        f = lax.dot_general(x[:, 256:], xw[:, 128:], contract, preferred_element_type=jnp.float32)
        finish(2 * pair, g[128:192, :128], g[64:128, :128], rolled(g[:64, :128], HALF), g[128:192, 128:], 0)
        swapped = jnp.where(lane < HALF, f[64:, 128:], f[64:, :128])
        middle = jnp.where(lane < HALF, f[:64, 128:], f[:64, :128])
        finish(2 * pair + 1, rolled(swapped, HALF), rolled(middle, HALF), g[192:, 128:], f[64:, 128:], HALF)


def spread_weights(exp_ref, w_ref):
    for i in range(exp_ref.shape[0] // LANES):
        power = (1 << exp_ref[LANES * i : LANES * (i + 1)].reshape(1, LANES)).astype(jnp.float32)
        w_ref[LANES * i : LANES * (i + 1)] = jnp.broadcast_to(power, (LANES, LANES)).T.astype(jnp.bfloat16)


def their_grams_kernel(core_ref, xa_ref, xb_ref, exp_ref, o_ref, w_ref):
    i = pl.program_id(0)

    @pl.when(i == 0)
    def _():
        spread_weights(exp_ref, w_ref)

    for part, x_ref in enumerate((xa_ref, xb_ref)):
        base = BLOCK_ROWS * (2 * i + part) if o_ref.shape[0] > 2 * BLOCK_ROWS else BLOCK_ROWS * part

        def put(index, start, rows, base=base):
            o_ref[pl.ds(pl.multiple_of(base + BODY * index + start, 8), rows.shape[0])] = rows

        def put_diag(index, diag, base=base):
            o_ref[pl.ds(pl.multiple_of(base + 8 * BODY, 8) + index, 1)] = diag

        block_grams(x_ref, w_ref, put, put_diag)


def their_grams(projected, weight_exp, core, half):
    tokens = projected.shape[0]
    x_spec = lambda part: pl.BlockSpec(
        (tokens, 8 * HD), lambda i, core: (0, 2 * chunk_block(half, 2 * i + part) + 1 - core[0])
    )
    return pl.pallas_call(
        their_grams_kernel,
        grid_spec=pltpu.PrefetchScalarGridSpec(
            num_scalar_prefetch=1,
            grid=(2,),
            in_specs=[x_spec(0), x_spec(1), pl.BlockSpec((tokens,), lambda i, core: (0,))],
            out_specs=pl.BlockSpec((2 * BLOCK_ROWS, LANES), lambda i, core: (i, 0)) if half else WHOLE,
            scratch_shapes=[pltpu.VMEM((tokens, LANES), jnp.bfloat16)],
        ),
        out_shape=(pltpu.HBM if half else pltpu.VMEM)((4 * BLOCK_ROWS, LANES), jnp.float32),
        compiler_params=params(16, dimension_semantics=("arbitrary",)),
        cost_estimate=pl.CostEstimate(flops=tokens * 64 * HD * HD, bytes_accessed=7_500_000, transcendentals=0),
        name="their_grams",
    )(core, off_chip(projected), off_chip(projected), off_chip(weight_exp))


def fill_slots(half, core_ref, x_refs, exp_ref, received_ref, all_ref, w_ref, packed=lambda spots: None):
    i = pl.program_id(0)

    @pl.when(i == 0)
    def _():
        spread_weights(exp_ref, w_ref)
        for slot in range(8):
            all_ref[slot, SLOT_ROWS - 8 :] = jnp.zeros((8, LANES), jnp.float32)

    spots = []
    for part, x_ref in enumerate(x_refs):
        spots.append([spot(chunk_block(half, 2 * i + part), inner, core_ref[0]) for inner in range(8)])

        def put(index, start, rows, part=part):
            slot, rest = spots[part][index]
            at = pl.ds(pl.multiple_of(BODY * rest + start, 8), rows.shape[0])
            source = BLOCK_ROWS * part + BODY * index + start
            all_ref[slot, at] = rows + received_ref[source : source + rows.shape[0]]

        def put_diag(index, diag, part=part):
            slot, rest = spots[part][index]
            source = BLOCK_ROWS * part + 8 * BODY + index
            all_ref[slot, pl.ds(4 * BODY + rest, 1)] = diag + received_ref[source : source + 1]

        block_grams(x_ref, w_ref, put, put_diag)
        packed(spots[part])


def my_even_kernel(core_ref, spot_ref, xa_ref, xb_ref, exp_ref, received_ref, o_ref, w_ref, all_ref, sem):
    def packed(spots):
        for slot, rest in spots:
            rows = pl.ds(pl.multiple_of(BODY * rest, 8), BODY)
            pltpu.make_async_copy(all_ref.at[slot, rows], o_ref.at[slot, rows], sem).start()

    fill_slots(0, core_ref, (xa_ref, xb_ref), exp_ref, received_ref, all_ref, w_ref, packed)

    @pl.when(pl.program_id(0) == pl.num_programs(0) - 1)
    def _():
        rows = pl.ds(4 * BODY, 8)
        pltpu.make_async_copy(all_ref.at[:, rows], o_ref.at[:, rows], sem).start()
        pltpu.make_async_copy(all_ref, o_ref, sem).wait()


def my_odd_kernel(core_ref, spot_ref, xa_ref, xb_ref, exp_ref, received_ref, *refs):
    outs, (w_ref, all_ref) = refs[:8], refs[8:]
    fill_slots(1, core_ref, (xa_ref, xb_ref), exp_ref, received_ref, all_ref, w_ref)

    @pl.when(pl.program_id(0) == pl.num_programs(0) - 1)
    def _():
        for flip in range(8):
            outs[flip][...] = all_ref[spot_ref[0] ^ flip]


def my_grams(projected, weight_exp, received, core, own_spot, half):
    tokens = projected.shape[0]
    scratch = [pltpu.VMEM((tokens, LANES), jnp.bfloat16), pltpu.VMEM((8, SLOT_ROWS, LANES), jnp.float32)]
    if half:
        kernel, outs = my_odd_kernel, [WHOLE] * 8
        shapes = [pltpu.VMEM((SLOT_ROWS, LANES), jnp.float32)] * 8
    else:
        kernel, outs = my_even_kernel, pl.BlockSpec(memory_space=pl.ANY)
        shapes = pltpu.HBM((8, SLOT_ROWS, LANES), jnp.float32)
        scratch.append(pltpu.SemaphoreType.DMA(()))
    x_spec = lambda part: pl.BlockSpec(
        (tokens, 8 * HD), lambda i, core, spot: (0, 2 * chunk_block(half, 2 * i + part) + core[0])
    )
    return pl.pallas_call(
        kernel,
        grid_spec=pltpu.PrefetchScalarGridSpec(
            num_scalar_prefetch=2,
            grid=(2,),
            in_specs=[
                x_spec(0),
                x_spec(1),
                pl.BlockSpec((tokens,), lambda i, core, spot: (0,)),
                pl.BlockSpec((2 * BLOCK_ROWS, LANES), lambda i, core, spot: (i, 0)),
            ],
            out_specs=outs,
            scratch_shapes=scratch,
        ),
        out_shape=shapes,
        compiler_params=params(20, dimension_semantics=("arbitrary",)),
        cost_estimate=pl.CostEstimate(flops=tokens * 64 * HD * HD, bytes_accessed=10_000_000, transcendentals=0),
        name="my_grams",
    )(core, own_spot, off_chip(projected), off_chip(projected), off_chip(weight_exp), off_chip(received))


def even_kernel(even_ref, o_ref):
    def one(i, carry):
        rows = pl.ds(pl.multiple_of(8 * i, 8), 8)
        total = even_ref[0, rows]
        for k in range(1, 8):
            total = total + even_ref[k, rows]
        o_ref[rows] = total
        return carry

    lax.fori_loop(0, SLOT_ROWS // 8, one, 0, unroll=8)


def add_even(even):
    return pl.pallas_call(
        even_kernel,
        in_specs=[WHOLE],
        out_specs=WHOLE,
        out_shape=pltpu.VMEM((SLOT_ROWS, LANES), jnp.float32),
        compiler_params=params(8),
        cost_estimate=pl.CostEstimate(flops=6_000_000, bytes_accessed=3_000_000, transcendentals=0),
        name="add_even",
    )(off_chip(even))


def odd_kernel(even_ref, *refs):
    odd_refs, o_ref = refs[:8], refs[8]
    for i in range(4):
        rows = slice(BODY * i, BODY * (i + 1))
        o_ref[i, :BODY] = even_ref[rows]
        total = odd_refs[0][rows]
        for k in range(1, 8):
            total = total + odd_refs[k][rows]
        o_ref[4 + i, :BODY] = total
    last = slice(4 * BODY, SLOT_ROWS)
    total = odd_refs[0][last]
    for k in range(1, 8):
        total = total + odd_refs[k][last]
    for half, diags in enumerate((even_ref[last], total)):
        for i in range(4):
            o_ref[4 * half + i, BODY:] = jnp.broadcast_to(diags[i : i + 1], (8, LANES))


def add_odd(even_sum, odd):
    return pl.pallas_call(
        odd_kernel,
        in_specs=[WHOLE] * 9,
        out_specs=WHOLE,
        out_shape=pltpu.VMEM((8, ROWS, LANES), jnp.float32),
        compiler_params=params(8),
        name="add_odd",
    )(on_chip(even_sum), *[on_chip(v) for v in odd])


def mm(a, b, dims=((1,), (0,))):
    return lax.dot_general(a, b, (dims, ((), ())), precision=lax.Precision.HIGHEST, preferred_element_type=jnp.float32)


def factor(block, row, lane):
    m = jnp.where(lane - HALF == row, 1.0, block)
    tiles = [m[8 * t : 8 * t + 8] for t in range(8)]
    sub = lax.broadcasted_iota(jnp.int32, (8, LANES), 0)
    wide = lambda v: jnp.broadcast_to(v, (8, LANES))
    out = []
    for t in range(0, 8, PANEL):
        size = 8 * PANEL
        cols = {v: [wide(tiles[v][:, 8 * t + j : 8 * t + j + 1]) for j in range(size)] for v in range(t, 8)}
        q = []
        for j in range(size):
            own, k = t + j // 8, j % 8
            c, d = cols[own], tiles[own]
            r = 1.0 / c[j][k : k + 1]
            out.append(d[k : k + 1] * lax.rsqrt(c[j][k : k + 1]))
            q.append(wide(d[k : k + 1] * r))
            u = {l: wide(c[l][k : k + 1] * r) for l in range(j + 1, size)}
            for v in range(own, 8):
                part = jnp.where(sub > k, cols[v][j], 0.0) if v == own else cols[v][j]
                if v < t + PANEL:
                    tiles[v] = tiles[v] - part * q[j]
                for l in range(j + 1, size):
                    cols[v][l] = cols[v][l] - part * u[l]
        for v in range(t + PANEL, 8):
            for j in range(size):
                tiles[v] = tiles[v] - cols[v][j] * q[j]
    return jnp.concatenate(out, axis=0)


def whiten_kernel(index_ref, damp_ref, g_ref, o_ref):
    packed = g_ref[0]
    for i in range(1, 8):
        packed = packed + g_ref[i]
    packed = packed / TOKENS
    row = lax.broadcasted_iota(jnp.int32, (HALF, LANES), 0)
    lane = lax.broadcasted_iota(jnp.int32, (HALF, LANES), 1)
    row32, lane32 = row[:32], lane[:32]
    low = packed[0:64]
    mid = packed[64:128]
    tail = packed[128:144]
    extra = jnp.broadcast_to(packed[144:145], (HALF, LANES))
    turned = rolled(mid, HALF)
    inside = lane < HALF
    upper00 = jnp.where((lane > row) & inside, turned, 0.0)
    lower11 = jnp.where((lane < row), turned, 0.0)
    diag11 = jnp.where(lane == row, turned, 0.0)
    folded = jnp.concatenate([tail, rolled(tail, HALF)], axis=0)
    h10 = jnp.where(lane32 < 32, folded, 0.0)
    fturn = rolled(folded, LANES - 32)
    hup = jnp.where((lane32 > row32) & (lane32 < 32), fturn, 0.0)
    hlow = jnp.where(lane32 < row32, fturn, 0.0)
    hdiag = jnp.where(lane32 == row32, fturn, 0.0)
    extra_turned = rolled(extra, HALF)
    diag00 = jnp.where(lane == row, extra_turned, 0.0)
    hdiag0 = jnp.where(lane32 == row32, extra[:32], 0.0)
    lower22 = jnp.concatenate([jnp.zeros((32, LANES), jnp.float32), h10 + jnp.where(lane32 >= 32, rolled(hlow, 32), 0.0)], axis=0)
    upper22 = jnp.concatenate([hup, jnp.zeros((32, LANES), jnp.float32)], axis=0)
    diag22 = jnp.concatenate([hdiag0, rolled(hdiag, 32)], axis=0)

    def flip(v):
        return jnp.concatenate([v.T[:HALF], jnp.zeros((HALF, HALF), jnp.float32)], axis=1)

    s00 = upper00 + flip(upper00) + diag00
    s11 = lower11 + flip(lower11) + diag11
    off22 = lower22 + upper22
    s22 = off22 + flip(off22) + diag22
    trace = jnp.sum(jnp.sum(diag00 + diag11 + diag22, axis=0, keepdims=True), axis=1, keepdims=True)
    scale = (1 << damp_ref[index_ref[0]]).astype(jnp.float32)
    damping = (trace / HD + 1e-6) / scale
    eye = jnp.where(lane == row, jnp.broadcast_to(damping, (HALF, LANES)), 0.0)
    s10 = mid[:, :HALF]
    s20, s21 = low[:, :HALF], low[:, HALF:]

    w0 = factor(s00 + eye, row, lane)[:, HALF:]
    u10 = mm(w0, s10, ((1,), (1,)))
    u20 = mm(w0, s20, ((1,), (1,)))
    pad = jnp.zeros((HALF, HALF), jnp.float32)
    r11 = s11 + eye - jnp.concatenate([mm(u10, u10, ((0,), (0,))), pad], axis=1)
    r21 = s21 - mm(u20, u10, ((0,), (0,)))
    w1 = factor(r11, row, lane)[:, HALF:]
    u21 = mm(w1, r21, ((1,), (1,)))
    gap = mm(u20, u20, ((0,), (0,))) + mm(u21, u21, ((0,), (0,)))
    r22 = s22 + eye - jnp.concatenate([gap, pad], axis=1)
    x10 = mm(u10, w0, ((0,), (0,)))
    w10 = -mm(w1, x10)
    x20 = mm(u20, w0, ((0,), (0,))) + mm(u21, w10, ((0,), (0,)))
    x21 = mm(u21, w1, ((0,), (0,)))
    w2 = factor(r22, row, lane)[:, HALF:]
    low_out = -mm(w2, jnp.concatenate([x20, x21], axis=1))

    def twice(v):
        return jnp.concatenate([v, v], axis=1)

    turned0 = twice(w0).T
    turned0 = jnp.concatenate([turned0[:HALF], turned0[HALF:]], axis=1)
    middle = jnp.where(lane - HALF > row, turned0, jnp.concatenate([w10, w1], axis=1))
    w2_wide = twice(w2)
    corner = w2_wide[:32]
    corner = jnp.concatenate([corner] * 4, axis=0).T[:32]
    tri = jnp.where((lane32 & 63) - 32 > row32, corner, w2_wide[32:])
    tri = jnp.where(lane[:16] < HALF, tri[:16], tri[16:])
    diag = jnp.sum(jnp.where(lane == row, twice(w0), 0.0), axis=0, keepdims=True)
    diag += jnp.sum(jnp.where(lane32 - HALF == row32, w2_wide[:32], 0.0), axis=0, keepdims=True)
    for i in range(8):
        o_ref[i, 0:64] = low_out
        o_ref[i, 64:128] = middle
        o_ref[i, 128:144] = tri
        o_ref[i, 144:152] = jnp.broadcast_to(diag, (8, LANES))


def whiten(index, damp_exp, parts):
    smem = pl.BlockSpec(memory_space=pltpu.SMEM)
    return pl.pallas_call(
        whiten_kernel,
        in_specs=[smem, smem, WHOLE],
        out_specs=WHOLE,
        out_shape=pltpu.VMEM((8, ROWS, LANES), jnp.float32),
        compiler_params=params(8),
        name="whiten",
    )(index, damp_exp, on_chip(parts))


def spread_kernel(p_ref, o_ref):
    row = lax.broadcasted_iota(jnp.int32, (HALF, LANES), 0)
    lane = lax.broadcasted_iota(jnp.int32, (HALF, LANES), 1)
    row32, lane32 = row[:32], lane[:32]
    first_matrix = o_ref.shape[0] * pl.program_id(0)
    for i in range(o_ref.shape[0]):
        middle = p_ref[first_matrix + i, 64:128]
        tail = p_ref[first_matrix + i, 128:144]
        diag = p_ref[first_matrix + i, 144:145]
        turned = jnp.concatenate([middle, middle], axis=0).T[HALF:]
        first = jnp.where(lane < row, turned, jnp.where(lane == row, diag, 0.0))
        o_ref[i, 0:64, 0:128] = first
        o_ref[i, 64:128, 0:128] = jnp.where(lane - HALF <= row, middle, 0.0)
        o_ref[i, 128:192, 0:128] = p_ref[first_matrix + i, 0:64]
        o_ref[i, 0:128, 128:192] = jnp.zeros((128, HALF), jnp.float32)
        lower = jnp.concatenate([tail, rolled(tail, HALF)], axis=0)
        corner = jnp.concatenate([lower] * 4, axis=0).T[32:64]
        corner_diag = rolled(jnp.broadcast_to(diag, (32, LANES)), HALF)
        top = jnp.where(lane32 < row32, corner, jnp.where(lane32 == row32, corner_diag, 0.0))
        bottom = jnp.where(lane32 - 32 <= row32, lower, 0.0)
        o_ref[i, 128:160, 128:192] = top[:, :HALF]
        o_ref[i, 160:192, 128:192] = bottom[:, :HALF]


def spread(packed):
    return pl.pallas_call(
        spread_kernel,
        grid=(2,),
        in_specs=[WHOLE],
        out_specs=pl.BlockSpec((4, HD, HD), lambda i: (i, 0, 0)),
        out_shape=jax.ShapeDtypeStruct((8, HD, HD), jnp.float32),
        compiler_params=params(8),
        name="spread",
    )(on_chip(packed))


def on_device(projected, weight_exp, damp_exp):
    dp, head = lax.axis_index("dp"), lax.axis_index("head")
    core = head % 2
    x, z, y_lo, y_hi = head // 4, dp % 4, dp // 4, head // 2 % 2
    y = 2 * y_hi + y_lo
    a = near(x) * 4 + near(y) * 2 + near(z)
    b = far(x) * 4 + far(y) * 2 + far(z)
    core, own_spot = core[None], jnp.where(core == 0, b, a)[None]
    theirs = [their_grams(projected, weight_exp, core, half) for half in range(2)]
    received = [lax.ppermute(part, DEVICES, partner_pairs()) for part in theirs]
    even = my_grams(projected, weight_exp, received[0], core, own_spot, 0)
    even = lax.all_to_all(even, DEVICES, 0, 0, tiled=True, axis_index_groups=cubes(0))
    odd = my_grams(projected, weight_exp, received[1], core, own_spot, 1)
    swapped = [odd[0]]
    for flip in range(1, 8):
        swapped.append(lax.ppermute(odd[flip], DEVICES, peers(flip)))
    even_sum = add_even(even)
    cube = add_odd(even_sum, swapped)
    parts = lax.all_to_all(cube, DEVICES, 0, 0, tiled=True, axis_index_groups=cubes(1))
    factors = whiten((head * 8 + dp)[None], damp_exp, parts)
    gathered = lax.all_to_all(factors, DEVICES, 0, 0, tiled=True, axis_index_groups=owner_groups())
    return spread(gathered)


def solution(mesh):
    return jax.shard_map(
        on_device,
        mesh=mesh,
        in_specs=(P(("dp", "head"), None), P(("dp", "head")), P()),
        out_specs=P("head", None, None),
        check_vma=False,
    )
```
